128 devices in a mesh: dp: 32 (over z, x, core), tensor: 4 (over y).
Axes of the slice: x: 4, y: 4, z: 4, core: 2. Of those that a mesh axis runs over, the one named last changes fastest.
Arguments:
- activations: bfloat16 [64, 128, 4096], P('dp'), may hold values from -6 to 6
- out_grads: bfloat16 [64, 128, 20480], P('dp', None, 'tensor'), may hold values from -0.625 to 0.625
- act_scale: bfloat16 [64, 32], P('dp'), may hold values from 1 to 16
- grad_scale: bfloat16 [64, 1, 20480], P('dp', None, 'tensor'), may hold values from 1 to 72
- moment: float32 [20480, 4096], P(('tensor', 'dp')), may hold values from -0.6 to 0.6
- second: float32 [20480, 4096], P(('tensor', 'dp')), may hold values from 0.1 to 1
- master: float32 [20480, 4096], P(('tensor', 'dp')), may hold values from -0.0625 to 0.0625
Outputs:
- new_moment: float32 [20480, 4096], P(('tensor', 'dp'))
- new_second: float32 [20480, 4096], P(('tensor', 'dp'))
- new_master: float32 [20480, 4096], P(('tensor', 'dp'))
- weights: bfloat16 [20480, 4096], P(('tensor', 'dp'))
The draws below stay inside these ranges and needn't reach their ends.
All inputs are finite; a program needn't handle non-finite values.
Results may differ from the reference program's by a relative error of at most 0.015.
Values may be sent and summed in bfloat16 or wider, within the bound.
A program may use at most 192 MiB of HBM per device.

```python
import math
import jax
import jax.numpy as jnp
from jax import lax

FF = 20480
ROWS = 4096
TILE = 128
TOK_DEV = 256
TOKENS = 8192
BLOCKS = 64
N_DP = 32


def draw_act_scale(key, part):
    upper = math.log(10.0)
    values = jnp.exp(jax.random.uniform(key, (BLOCKS, ROWS // TILE), jnp.float32, 0.0, upper))
    return values.astype(jnp.bfloat16)


def draw_grad_scale(key, part):
    upper = math.log(4.0)
    columns = jnp.arange(FF, dtype=jnp.float32) / (FF - 1)
    riser = jnp.exp(columns * math.log(9.0))
    base = jnp.exp(jax.random.uniform(key, (BLOCKS, 1, FF), jnp.float32, 0.0, upper))
    return (base * riser[None, None, :]).astype(jnp.bfloat16)


def with_spikes(values, rng, source, target, parts, factor):
    owner, partner = [(jnp.arange(values.shape[axis_at]) // (values.shape[axis_at] // parts)).reshape([-1 if axis == axis_at else 1 for axis in range(values.ndim)]) for axis_at in (source, target)]
    chosen = jax.random.permutation(rng, parts)[partner]
    strong = (owner == chosen) | (owner == (partner + parts // 2) % parts)
    return jnp.where(strong, factor * values, values)


def steps_of(key, extent, split, least, largest):
    gain, own = 1.0, jax.random.fold_in(key, 6)
    for dim, blocks in split:
        draws = jnp.exp(jax.random.uniform(jax.random.fold_in(own, dim), (blocks,), jnp.float32, least / len(split), largest / len(split)))
        gain = gain * jnp.repeat(draws, extent[dim] // blocks).reshape([-1 if axis == dim else 1 for axis in range(len(extent))])
    return gain


def scatter_about(rng, extent, scale, most, pieces=(), held_as=jnp.bfloat16):
    level = steps_of(rng, extent, pieces, -0.22, 0.18) if pieces else 1.0
    drawn = jax.random.normal(rng, extent, jnp.float32) * scale * level
    return jnp.minimum(jnp.maximum(drawn, -most), most).astype(held_as)


def gaussian_with(key, shape, deviation, reach, pieces, heavy, kind=jnp.bfloat16):
    entries = deviation * jax.random.normal(key, shape, jnp.float32)
    if pieces:
        entries = entries * steps_of(key, shape, pieces, -0.22, 0.18)
    return jnp.clip(with_spikes(entries, jax.random.fold_in(key, 3), *heavy), -reach, reach).astype(kind)


def setup_inputs(seed: int = 0) -> dict:
    streams_of = jax.random.split(jax.random.key(seed), 8)
    activations = scatter_about(streams_of[0], (BLOCKS, TILE, ROWS), 1.0, 6.0, ((0, 32),))
    out_grads = gaussian_with(streams_of[1], (BLOCKS, TILE, FF), (2.0 / TOKENS ** 0.5), 0.625, ((0, 32), (2, 4)), (0, 2, 32, 2.75))
    act_scale = draw_act_scale(jax.random.fold_in(streams_of[7], 71), 0)
    grad_scale = draw_grad_scale(jax.random.fold_in(streams_of[7], 71), 0)
    moment = scatter_about(streams_of[4], (FF, ROWS), 0.1, 0.6, ((0, 128),), jnp.float32)
    second = jnp.clip(jnp.exp(math.log(1.0) - 2.3025851 * jax.random.uniform(streams_of[5], (FF, ROWS), jnp.float32) ** steps_of(streams_of[5], (FF, ROWS), ((0, 128),), -0.2, 0.2)), 0.1, 1.0)
    master = scatter_about(streams_of[6], (FF, ROWS), 8192 ** -0.5, 0.0625, ((0, 128),), jnp.float32)
    return dict(activations=activations, out_grads=out_grads, act_scale=act_scale, grad_scale=grad_scale, moment=moment, second=second, master=master)


clip_rms = 1.0
beta_first = 0.9
beta_second = 0.95
learn_rate = 0.003
adam_eps = 1e-08

def widen(act_scale):
    tiles = act_scale.astype(jnp.float32)
    spread = jnp.broadcast_to(tiles[:, :, None], tiles.shape + (TILE,))
    return spread.reshape(tiles.shape[0], tiles.shape[1] * TILE)

def reference(activations, out_grads, act_scale, grad_scale, moment, second, master):
    acts_deq = (activations.astype(jnp.float32) * widen(act_scale)[:, None, :]).astype(jnp.bfloat16).reshape(TOKENS, ROWS)
    grads_deq = (out_grads.astype(jnp.float32) * grad_scale.astype(jnp.float32)).astype(jnp.bfloat16).reshape(TOKENS, FF)

    def add_group(group, total):
        start = (group * TOK_DEV).astype(jnp.int32)
        grads_group = lax.dynamic_slice_in_dim(grads_deq, start, TOK_DEV, 0)
        acts_group = lax.dynamic_slice_in_dim(acts_deq, start, TOK_DEV, 0)
        term = jnp.dot(grads_group.T, acts_group, preferred_element_type=jnp.float32)
        rounded = lax.optimization_barrier(term.astype(jnp.bfloat16))
        return total + rounded.astype(jnp.float32)
    grad = lax.fori_loop(0, N_DP, add_group, jnp.zeros((FF, ROWS), jnp.float32))
    norm = jnp.sqrt(jnp.sum(grad * grad))
    factor = jnp.minimum(1.0, clip_rms * jnp.sqrt(jnp.float32(FF * ROWS)) / norm)
    clipped = factor * grad
    new_moment = beta_first * moment + (1.0 - beta_first) * clipped
    new_second = beta_second * second + (1.0 - beta_second) * clipped * clipped
    new_master = master - learn_rate * new_moment / (jnp.sqrt(new_second) + adam_eps)
    weights = new_master.astype(jnp.bfloat16)
    return (new_moment, new_second, new_master, weights)
```

```python
import functools

import jax
import jax.numpy as jnp
from jax import lax
from jax.experimental import pallas as pl
from jax.experimental.pallas import tpu as pltpu
from jax.sharding import Mesh
from jax.sharding import PartitionSpec as P

FF = 20480
ROWS = 4096
DP = ("dp_0", "dp_1", "dp_2")
TENSOR_DP = ("tensor", "dp_0", "dp_1", "dp_2")

clip_rms = 1.0
beta_first = 0.9
beta_second = 0.95
learn_rate = 0.003
adam_eps = 1e-08

TOK = 256
HALF = ROWS // 2
TILE = 256
STEPS = HALF // TILE
BLK = 320
OWN = 160
QUART = 128
B_OFF = (2, 1, 3, 0)
BF = jnp.bfloat16
F32 = jnp.float32


def kernel(
    acts_hbm, grads_hbm, ascale, gscale,
    grad_out, factor_out,
    acts_raw, grads_raw, wide, A, S, GO, G, RB, PB, H, RF, PP, acc, NS, N1, N2, N3,
    load_sem, pair_s, pair_r, q_s, q_r, d_s, d_r, y_s, y_r,
    hop_s, hop_r, nbr_s, nbr_r, rel_s, rel_r,
    rh_s, rh_r, rf_s, rf_r, pp_s, pp_r, n_s, n_r,
):
    z = lax.axis_index("dp_0")
    x = lax.axis_index("dp_1")
    c = lax.axis_index("dp_2")
    y = lax.axis_index("tensor")
    a = x + c * (z - x)
    b = z + c * (x - z)

    def gdev(d):
        return (lax.rem(z + c * d, 4), lax.rem(x + (1 - c) * d, 4), c, y)

    def rdev(d, core):
        return (lax.rem(z + (1 - c) * d, 4), lax.rem(x + c * d, 4), core, y)

    def ydev(d):
        return (z, x, c, lax.rem(y + d, 4))

    partner = (z, x, 1 - c, y)
    MESH = pl.DeviceIdType.MESH

    def send(src, dst, ss, rs, dev):
        pltpu.make_async_remote_copy(
            src_ref=src, dst_ref=dst, send_sem=ss, recv_sem=rs, device_id=dev, device_id_type=MESH
        ).start()

    def wait(ref, sem):
        pltpu.make_async_copy(ref, ref, sem).wait()

    def of(i, n):
        return pl.ds(pl.multiple_of(i, n), n)

    load_a = pltpu.make_async_copy(acts_hbm, acts_raw, load_sem.at[0])
    load_g = pltpu.make_async_copy(grads_hbm, grads_raw, load_sem.at[1])
    load_a.start()
    load_g.start()
    barrier = pltpu.get_barrier_semaphore()
    greet = [partner]
    for d in (1, 3):
        for core in (0, 1):
            greet.append((lax.rem(z + d, 4), x, core, y))
            greet.append((z, lax.rem(x + d, 4), core, y))
        greet.append(ydev(d))
    for core in (0, 1):
        greet.append((lax.rem(z + 2, 4), x, core, y))
    greet.append((z, lax.rem(x + 2, 4), c, y))
    greet.append(ydev(2))
    for dev in greet:
        pl.semaphore_signal(barrier, inc=1, device_id=dev, device_id_type=MESH)

    for r in range(ROWS // 128):
        wide[:, r * 128 : (r + 1) * 128] = jnp.broadcast_to(
            ascale[:, r : r + 1].astype(F32), (2, 128)
        )
    load_a.wait()

    def scale_acts(i, which, put):
        cols = pl.ds(pl.multiple_of(which * HALF + i * 512, 512), 512)
        for blk in range(2):
            rows = slice(blk * 128, blk * 128 + 128)
            put(blk, i, (acts_raw[blk, :, cols].astype(F32) * wide[blk : blk + 1, cols]).astype(BF))

    def put_other(blk, i, v):
        S[blk * 128 : blk * 128 + 128, pl.ds(pl.multiple_of(i * 512, 512), 512)] = v

    def put_own(blk, i, v):
        A[0, of(c * TOK + blk * 128, 128), pl.ds(pl.multiple_of(i * 512, 512), 512)] = v

    def other_step(i, _):
        scale_acts(i, 1 - c, put_other)
        return 0

    def own_step(i, _):
        scale_acts(i, c, put_own)
        return 0

    lax.fori_loop(0, HALF // 512, other_step, 0)
    pl.semaphore_wait(barrier, len(greet))
    send(S, A.at[0, of(c * TOK, TOK)], pair_s.at[0], pair_r.at[0], partner)
    lax.fori_loop(0, HALF // 512, own_step, 0)
    wait(A.at[0, of((1 - c) * TOK, TOK)], pair_r.at[0])

    mine = of(y * QUART, QUART)
    lo64 = pl.ds(pl.multiple_of(y * QUART, 64), 64)
    hi64 = pl.ds(pl.multiple_of(y * QUART + 64, 64), 64)
    groups = (pl.ds(TILE, TILE), pl.ds(2 * TILE, HALF - 2 * TILE))

    def q_own(g):
        cols = groups[g]
        send(A.at[0, mine, cols], A.at[3, mine, cols], q_s.at[g, 0], q_r.at[g, 0], gdev(1))
        send(A.at[0, mine, cols], A.at[1, mine, cols], q_s.at[g, 1], q_r.at[g, 1], gdev(3))

    def q_relay(g):
        cols = groups[g]
        wait(A.at[3, mine, cols], q_r.at[g, 0])
        send(A.at[3, lo64, cols], A.at[2, lo64, cols], q_s.at[g, 2], q_r.at[g, 2], gdev(1))
        wait(A.at[1, mine, cols], q_r.at[g, 1])
        send(A.at[1, hi64, cols], A.at[2, hi64, cols], q_s.at[g, 3], q_r.at[g, 3], gdev(3))

    def q_done(g):
        cols = groups[g]
        wait(A.at[2, lo64, cols], q_r.at[g, 2])
        wait(A.at[2, hi64, cols], q_r.at[g, 3])

    def q_drain(g):
        cols = groups[g]
        wait(A.at[0, mine, cols], q_s.at[g, 0])
        wait(A.at[0, mine, cols], q_s.at[g, 1])
        wait(A.at[3, lo64, cols], q_s.at[g, 2])
        wait(A.at[1, hi64, cols], q_s.at[g, 3])

    def tile(t):
        return pl.ds(pl.multiple_of(t * TILE, TILE), TILE)

    three = pl.ds(1, 3)
    below = lax.rem(y + 3, 4)
    above = lax.rem(y + 1, 4)
    y_lo = pl.ds(pl.multiple_of(below * QUART, 64), 64)
    y_hi = pl.ds(pl.multiple_of(above * QUART + 64, 64), 64)
    far = lax.rem(y + 2, 4)
    f_lo = pl.ds(pl.multiple_of(far * QUART, 64), 64)
    f_hi = pl.ds(pl.multiple_of(far * QUART + 64, 64), 64)

    def y_own(u):
        v = A.at[three, mine, tile(u)]
        send(v, v, y_s.at[u, 0], y_r.at[u, 0], ydev(1))
        send(v, v, y_s.at[u, 1], y_r.at[u, 1], ydev(3))

    def y_relay(u):
        wait(A.at[three, of(below * QUART, QUART), tile(u)], y_r.at[u, 0])
        v = A.at[three, y_lo, tile(u)]
        send(v, v, y_s.at[u, 2], y_r.at[u, 2], ydev(1))
        wait(A.at[three, of(above * QUART, QUART), tile(u)], y_r.at[u, 1])
        v = A.at[three, y_hi, tile(u)]
        send(v, v, y_s.at[u, 3], y_r.at[u, 3], ydev(3))

    def y_done(u):
        wait(A.at[three, f_lo, tile(u)], y_r.at[u, 2])
        wait(A.at[three, f_hi, tile(u)], y_r.at[u, 3])

    def y_drain(u):
        wait(A.at[three, mine, tile(u)], y_s.at[u, 0])
        wait(A.at[three, mine, tile(u)], y_s.at[u, 1])
        wait(A.at[three, y_lo, tile(u)], y_s.at[u, 2])
        wait(A.at[three, y_hi, tile(u)], y_s.at[u, 3])

    q_own(0)
    q_own(1)

    load_g.wait()

    def turn(i, _):
        cols = pl.ds(pl.multiple_of(i * 512, 512), 512)
        for blk in range(2):
            v = grads_raw[blk, :, cols].astype(F32) * gscale[blk, :, cols].astype(F32)
            GO[cols, of(c * TOK + blk * 128, 128)] = v.T.astype(BF)
        return 0

    lax.fori_loop(0, 10, turn, 0)
    send(GO.at[:, of(c * TOK, TOK)], GO.at[:, of(c * TOK, TOK)], pair_s.at[1], pair_r.at[1], partner)

    q_relay(0)
    q_relay(1)
    d_cols = pl.ds(0, TILE)
    send(A.at[0, :, d_cols], A.at[3, :, d_cols], d_s.at[0], d_r.at[0], gdev(1))
    send(A.at[0, :, d_cols], A.at[1, :, d_cols], d_s.at[1], d_r.at[1], gdev(3))
    q_done(0)
    y_own(1)

    wait(GO.at[:, of((1 - c) * TOK, TOK)], pair_r.at[1])

    def block(da, p, part, n):
        aa = lax.rem(a + da, 4)
        bb = lax.rem(b + B_OFF[p], 4)
        start = (bb * 4 + aa + c * 3 * (aa - bb)) * BLK + part * OWN
        return pl.ds(pl.multiple_of(start, OWN), n)

    for p in range(4):
        send(GO.at[block(2, p, 0, OWN)], RB.at[0, p], hop_s.at[0, p], hop_r.at[0, p], gdev(1))
        send(GO.at[block(2, p, 1, OWN)], RB.at[1, p], hop_s.at[1, p], hop_r.at[1, p], gdev(3))
    own_copies = [
        pltpu.make_async_copy(GO.at[block(0, p, 0, BLK)], G.at[p, :, pl.ds(0, 512)], load_sem.at[2 + p])
        for p in range(4)
    ]
    for cp in own_copies:
        cp.start()

    q_done(1)
    for u in range(2, STEPS):
        y_own(u)

    d_lo, d_hi = pl.ds(0, 256), pl.ds(256, 256)
    wait(A.at[3, :, d_cols], d_r.at[0])
    send(A.at[3, d_lo, d_cols], A.at[2, d_lo, d_cols], d_s.at[2], d_r.at[2], gdev(1))
    wait(A.at[1, :, d_cols], d_r.at[1])
    send(A.at[1, d_hi, d_cols], A.at[2, d_hi, d_cols], d_s.at[3], d_r.at[3], gdev(3))

    for p in range(4):
        src = GO.at[block(1, p, 0, BLK)]
        send(src, G.at[p, :, pl.ds(1536, 512)], nbr_s.at[0, p], nbr_r.at[0, p], gdev(1))
        src = GO.at[block(3, p, 0, BLK)]
        send(src, G.at[p, :, pl.ds(512, 512)], nbr_s.at[1, p], nbr_r.at[1, p], gdev(3))

    y_relay(1)
    first, second = pl.ds(0, OWN), pl.ds(OWN, OWN)
    slot2 = pl.ds(1024, 512)
    for p in range(4):
        wait(RB.at[0, p], hop_r.at[0, p])
        wait(RB.at[1, p], hop_r.at[1, p])
    send(RB.at[0], G.at[:, first, slot2], rel_s.at[0], rel_r.at[0], gdev(1))
    send(RB.at[1], G.at[:, second, slot2], rel_s.at[1], rel_r.at[1], gdev(3))
    for u in range(2, STEPS):
        y_relay(u)

    for p in range(4):
        own_copies[p].wait()
        wait(G.at[p, :, pl.ds(1536, 512)], nbr_r.at[0, p])
        wait(G.at[p, :, pl.ds(512, 512)], nbr_r.at[1, p])
    wait(G.at[:, first, slot2], rel_r.at[0])
    wait(G.at[:, second, slot2], rel_r.at[1])
    wait(A.at[2, d_lo, d_cols], d_r.at[2])
    wait(A.at[2, d_hi, d_cols], d_r.at[3])
    acc[...] = jnp.zeros_like(acc)

    def out_tile(h, t):
        return pl.ds(pl.multiple_of(h * HALF + t * TILE, TILE), TILE)

    def product(p, t):
        acts = A[:, :, tile(t)].reshape(4 * 512, TILE)
        return jnp.dot(G[p], acts, preferred_element_type=F32).astype(BF)

    def reduce_send(d, part, core, t):
        src = PB.at[1 + d, pl.ds(part * OWN, OWN), tile(t)]
        send(src, RF.at[d, :, out_tile(c, t)], rf_s.at[d, core, t], rf_r.at[d, c, t], rdev(1 + 2 * d, core))

    def add_send(t):
        for d in (0, 1):
            wait(H.at[d, :, tile(t)], rh_r.at[d, t])
            rows = pl.ds(d * OWN, OWN)
            both = PB[1 + d, rows, tile(t)].astype(F32) + H[d, :, tile(t)].astype(F32)
            PB[1 + d, rows, tile(t)] = both.astype(BF)
            reduce_send(d, d, d, t)

    def finish(t):
        wait(PP.at[:, out_tile(1 - c, t)], pp_r.at[t])
        for h in (0, 1):
            cols = out_tile(h, t)
            wait(RF.at[0, :, cols], rf_r.at[0, h, t])
            wait(RF.at[1, :, cols], rf_r.at[1, h, t])
            g = PP[:, cols].astype(F32) + RF[0, :, cols].astype(F32) + RF[1, :, cols].astype(F32)
            grad_out[:, cols] = g
            sq = jnp.sum((g * g).reshape(OWN // 8, 8, TILE), axis=0)
            acc[...] += sq[:, :128] + sq[:, 128:]

    keep = of(c * OWN, OWN)
    give = of((1 - c) * OWN, OWN)

    def step(t, _):
        @pl.when(t >= 1)
        def _():
            y_done(t)

        PB[0, :, tile(t)] = product(0, t)
        send(PB.at[0, first, tile(t)], H.at[0, :, tile(t)], rh_s.at[0, t], rh_r.at[0, t], rdev(1, c))
        send(PB.at[0, second, tile(t)], H.at[1, :, tile(t)], rh_s.at[1, t], rh_r.at[1, t], rdev(3, c))
        PB[1, :, tile(t)] = product(1, t)
        reduce_send(0, 1, 1, t)
        PB[2, :, tile(t)] = product(2, t)
        reduce_send(1, 0, 0, t)
        PB[3, :, tile(t)] = product(3, t)
        send(PB.at[3, give, tile(t)], PP.at[:, out_tile(c, t)], pp_s.at[t], pp_r.at[t], partner)
        PP[:, out_tile(c, t)] = PB[3, keep, tile(t)]

        @pl.when(t >= 1)
        def _():
            add_send(t - 1)

        @pl.when(t >= 3)
        def _():
            finish(t - 3)

        return 0

    lax.fori_loop(0, STEPS, step, 0)
    add_send(STEPS - 1)

    def last(t, _):
        finish(t)
        return 0

    lax.fori_loop(STEPS - 3, STEPS, last, 0)

    NS[0] = acc[...]
    sent = []
    for dz in range(4):
        for dc in range(2):
            i = dz * 2 + dc
            if i:
                dev = (lax.rem(z + dz, 4), x, lax.rem(c + dc, 2), y)
                send(NS.at[0], N1.at[i - 1], n_s.at[i - 1], n_r.at[i - 1], dev)
                sent.append((0, i - 1))
    for i in range(7):
        wait(N1.at[i], n_r.at[i])
    NS[1] = NS[0] + jnp.sum(N1[...], axis=0)
    for i in range(3):
        dev = (z, lax.rem(x + i + 1, 4), c, y)
        send(NS.at[1], N2.at[i], n_s.at[7 + i], n_r.at[7 + i], dev)
        sent.append((1, 7 + i))
    for i in range(3):
        wait(N2.at[i], n_r.at[7 + i])
    NS[2] = NS[1] + jnp.sum(N2[...], axis=0)
    for i in range(3):
        send(NS.at[2], N3.at[i], n_s.at[10 + i], n_r.at[10 + i], ydev(i + 1))
        sent.append((2, 10 + i))

    wait(S, pair_s.at[0])
    wait(GO.at[:, of(c * TOK, TOK)], pair_s.at[1])
    q_drain(0)
    q_drain(1)
    wait(A.at[0, :, d_cols], d_s.at[0])
    wait(A.at[0, :, d_cols], d_s.at[1])
    wait(A.at[3, d_lo, d_cols], d_s.at[2])
    wait(A.at[1, d_hi, d_cols], d_s.at[3])
    for u in range(1, STEPS):
        y_drain(u)
    for p in range(4):
        wait(RB.at[0, p], hop_s.at[0, p])
        wait(RB.at[1, p], hop_s.at[1, p])
        wait(G.at[p, :, pl.ds(1536, 512)], nbr_s.at[0, p])
        wait(G.at[p, :, pl.ds(512, 512)], nbr_s.at[1, p])
    wait(RB.at[0], rel_s.at[0])
    wait(RB.at[1], rel_s.at[1])

    def drain(t, _):
        for d in (0, 1):
            wait(H.at[d, :, tile(t)], rh_s.at[d, t])
            for core in (0, 1):
                wait(H.at[d, :, tile(t)], rf_s.at[d, core, t])
        wait(H.at[0, :, tile(t)], pp_s.at[t])
        return 0

    lax.fori_loop(0, STEPS, drain, 0)
    for i in range(3):
        wait(N3.at[i], n_r.at[10 + i])
    total = jnp.sum(NS[2] + jnp.sum(N3[...], axis=0), keepdims=True)
    limit = clip_rms * jnp.sqrt(jnp.full((1, 1), FF * ROWS, F32))
    factor_out[...] = jnp.broadcast_to(jnp.minimum(1.0, limit / jnp.sqrt(total)), (8, 128))
    for i, k in sent:
        wait(NS.at[i], n_s.at[k])


def owned_gradient(activations, out_grads, act_scale, grad_scale):
    dma = pltpu.SemaphoreType.DMA
    vmem = pltpu.VMEM
    scratch = [
        vmem((2, 128, ROWS), BF),
        vmem((2, 128, 5120), BF),
        vmem((2, ROWS), F32),
        vmem((4, 512, HALF), BF),
        vmem((TOK, HALF), BF),
        vmem((5120, 512), BF),
        vmem((4, BLK, 2048), BF),
        vmem((2, 4, OWN, 512), BF),
        vmem((4, BLK, HALF), BF),
        vmem((2, OWN, HALF), BF),
        vmem((2, OWN, ROWS), BF),
        vmem((OWN, ROWS), BF),
        vmem((8, 128), F32),
        vmem((3, 8, 128), F32),
        vmem((7, 8, 128), F32),
        vmem((3, 8, 128), F32),
        vmem((3, 8, 128), F32),
        dma((6,)),
        dma((2,)), dma((2,)),
        dma((2, 4)), dma((2, 4)),
        dma((4,)), dma((4,)),
        dma((STEPS, 4)), dma((STEPS, 4)),
        dma((2, 4)), dma((2, 4)),
        dma((2, 4)), dma((2, 4)),
        dma((2,)), dma((2,)),
        dma((2, STEPS)), dma((2, STEPS)),
        dma((2, 2, STEPS)), dma((2, 2, STEPS)),
        dma((STEPS,)), dma((STEPS,)),
        dma((13,)), dma((13,)),
    ]
    return pl.pallas_call(
        kernel,
        out_shape=(
            jax.ShapeDtypeStruct((OWN, ROWS), F32),
            jax.ShapeDtypeStruct((8, 128), F32),
        ),
        in_specs=[
            pl.BlockSpec(memory_space=pl.ANY),
            pl.BlockSpec(memory_space=pl.ANY),
            pl.BlockSpec(memory_space=vmem),
            pl.BlockSpec(memory_space=vmem),
        ],
        out_specs=(pl.BlockSpec(memory_space=vmem), pl.BlockSpec(memory_space=vmem)),
        scratch_shapes=scratch,
        compiler_params=pltpu.CompilerParams(
            collective_id=0, has_side_effects=True, vmem_limit_bytes=46 * 1024 * 1024
        ),
        cost_estimate=pl.CostEstimate(
            flops=2 * 8192 * OWN * ROWS, bytes_accessed=8 * 1024 * 1024, transcendentals=0
        ),
        name="owned_gradient",
    )(activations, out_grads, act_scale, grad_scale)


def per_device(activations, out_grads, act_scale, grad_scale, moment, second, master):
    grad_owned, factors = owned_gradient(activations, out_grads, act_scale, grad_scale)
    clipped = factors[0, 0] * grad_owned
    new_moment = beta_first * moment + (1.0 - beta_first) * clipped
    new_second = beta_second * second + (1.0 - beta_second) * clipped * clipped
    new_master = master - learn_rate * new_moment / (jnp.sqrt(new_second) + adam_eps)
    weights = new_master.astype(jnp.bfloat16)
    return (new_moment, new_second, new_master, weights)


def solution(mesh):
    finer = Mesh(
        mesh.devices.reshape(4, 4, 2, mesh.shape["tensor"]), ("dp_0", "dp_1", "dp_2", "tensor")
    )
    in_specs = (
        P(DP, None, None),
        P(DP, None, "tensor"),
        P(DP, None),
        P(DP, None, "tensor"),
        P(TENSOR_DP, None),
        P(TENSOR_DP, None),
        P(TENSOR_DP, None),
    )
    out_specs = (P(TENSOR_DP, None), P(TENSOR_DP, None), P(TENSOR_DP, None), P(TENSOR_DP, None))
    return jax.shard_map(
        per_device, mesh=finer, in_specs=in_specs, out_specs=out_specs, check_vma=False
    )
```

```python
import functools

import jax
import jax.numpy as jnp
from jax import lax
from jax.experimental import pallas as pl
from jax.experimental.pallas import tpu as pltpu
from jax.sharding import Mesh
from jax.sharding import PartitionSpec as P

FF = 20480
ROWS = 4096
DP = ("dp_0", "dp_1", "dp_2")
TENSOR_DP = ("tensor", "dp_0", "dp_1", "dp_2")

clip_rms = 1.0
beta_first = 0.9
beta_second = 0.95
learn_rate = 0.003
adam_eps = 1e-08

TOK = 256
HALF = ROWS // 2
TILE = 256
STEPS = HALF // TILE
BLK = 320
OWN = 160
QUART = 128
B_OFF = (2, 1, 3, 0)
BF = jnp.bfloat16
F32 = jnp.float32


def kernel(
    acts_hbm, grads_hbm, ascale_hbm, gscale_hbm,
    grad_out, factor_out,
    acts_raw, grads_raw, ascale, gscale, wide, A, S, GO, G, RB, PB, H, RF, PP, GR, acc, NS, N1, N2, N3,
    load_sem, own_sem, pair_s, pair_r, q_s, q_r, y_s, y_r,
    hop_s, hop_r, nbr_s, nbr_r, rel_s, rel_r,
    rh_s, rh_r, rf_s, rf_r, pp_s, pp_r, out_sem, n_s, n_r,
):
    z = lax.axis_index("dp_0")
    x = lax.axis_index("dp_1")
    c = lax.axis_index("dp_2")
    y = lax.axis_index("tensor")
    a = x + c * (z - x)
    b = z + c * (x - z)

    def gdev(d):
        return (lax.rem(z + c * d, 4), lax.rem(x + (1 - c) * d, 4), c, y)

    def rdev(d, core):
        return (lax.rem(z + (1 - c) * d, 4), lax.rem(x + c * d, 4), core, y)

    def ydev(d):
        return (z, x, c, lax.rem(y + d, 4))

    partner = (z, x, 1 - c, y)
    MESH = pl.DeviceIdType.MESH

    def send(src, dst, ss, rs, dev):
        pltpu.make_async_remote_copy(
            src_ref=src, dst_ref=dst, send_sem=ss, recv_sem=rs, device_id=dev, device_id_type=MESH
        ).start()

    def wait(ref, sem):
        pltpu.make_async_copy(ref, ref, sem).wait()

    def of(i, n):
        return pl.ds(pl.multiple_of(i, n), n)

    barrier = pltpu.get_barrier_semaphore()
    greet = [partner]
    for d in (1, 3):
        for core in (0, 1):
            greet.append((lax.rem(z + d, 4), x, core, y))
            greet.append((z, lax.rem(x + d, 4), core, y))
        greet.append(ydev(d))
    for dev in greet:
        pl.semaphore_signal(barrier, inc=1, device_id=dev, device_id_type=MESH)
    loads = [
        pltpu.make_async_copy(src, dst, load_sem.at[i])
        for i, (src, dst) in enumerate(
            ((ascale_hbm, ascale), (acts_hbm, acts_raw), (gscale_hbm, gscale), (grads_hbm, grads_raw))
        )
    ]
    for load in loads:
        load.start()

    loads[0].wait()
    for r in range(ROWS // 128):
        wide[:, r * 128 : (r + 1) * 128] = jnp.broadcast_to(
            ascale[:, r : r + 1].astype(F32), (2, 128)
        )
    loads[1].wait()

    def scale_step(i, _):
        dst = pl.ds(pl.multiple_of(i * 512, 512), 512)
        for which, put in ((1 - c, 0), (c, 1)):
            cols = pl.ds(pl.multiple_of(which * HALF + i * 512, 512), 512)
            for blk in range(2):
                v = (acts_raw[blk, :, cols].astype(F32) * wide[blk : blk + 1, cols]).astype(BF)
                v = v.reshape(2, 64, 512)
                rows = pl.ds(2 * blk, 2)
                if put:
                    A[0, c, rows, :, dst] = v
                else:
                    S[rows, :, dst] = v
        return 0

    lax.fori_loop(0, HALF // 512, scale_step, 0)

    def turn(i, _):
        cols = pl.ds(pl.multiple_of(i * 512, 512), 512)
        for blk in range(2):
            v = grads_raw[blk, :, cols].astype(F32) * gscale[blk : blk + 1, cols].astype(F32)
            GO[cols, of(c * TOK + blk * 128, 128)] = v.T.astype(BF)
        return 0

    pl.semaphore_wait(barrier, len(greet))

    groups = (pl.ds(0, TILE), pl.ds(TILE, 2 * TILE), pl.ds(3 * TILE, HALF - 3 * TILE))
    pieces = (pl.ds(0, TILE), pl.ds(TILE, HALF - TILE))
    for i in range(2):
        send(S.at[:, :, pieces[i]], A.at[0, c, :, :, pieces[i]], pair_s.at[i], pair_r.at[i], partner)

    def q_own(g, k):
        who = c + k * (1 - 2 * c)
        src = A.at[0, who, y, :, groups[g]]
        send(src, A.at[2, who, y, :, groups[g]], q_s.at[g, 0, k], q_r.at[g, 0, who], gdev(1))
        send(src, A.at[1, who, y, :, groups[g]], q_s.at[g, 1, k], q_r.at[g, 1, who], gdev(3))

    def q_relay(g):
        cols = groups[g]
        wait(A.at[2, 0, y, :, cols], q_r.at[g, 0, 0])
        send(A.at[2, 0, y, :, cols], A.at[3, 0, y, :, cols], q_s.at[g, 2, 0], q_r.at[g, 2, 0], gdev(1))
        wait(A.at[1, 1, y, :, cols], q_r.at[g, 1, 1])
        send(A.at[1, 1, y, :, cols], A.at[3, 1, y, :, cols], q_s.at[g, 2, 1], q_r.at[g, 2, 1], gdev(3))

    def q_near(g):
        cols = groups[g]
        wait(A.at[2, 1, y, :, cols], q_r.at[g, 0, 1])
        wait(A.at[1, 0, y, :, cols], q_r.at[g, 1, 0])

    def q_far(g):
        cols = groups[g]
        wait(A.at[3, 0, y, :, cols], q_r.at[g, 2, 0])
        wait(A.at[3, 1, y, :, cols], q_r.at[g, 2, 1])

    def q_drain(g):
        v = A.at[0, 0, y, :, groups[g]]
        for i in range(3):
            for k in range(2):
                wait(v, q_s.at[g, i, k])

    def tile(t):
        return pl.ds(pl.multiple_of(t * TILE, TILE), TILE)

    parts = (pl.ds(1, 2), pl.ds(3, 1))
    both = pl.ds(0, 2)
    below = lax.rem(y + 3, 4)
    above = lax.rem(y + 1, 4)
    far = lax.rem(y + 2, 4)

    def y_own(u, i):
        v = A.at[parts[i], both, y, :, tile(u)]
        send(v, v, y_s.at[u, i, 0], y_r.at[u, i, 0], ydev(1))
        send(v, v, y_s.at[u, i, 1], y_r.at[u, i, 1], ydev(3))

    def y_relay(u):
        for i in range(2):
            wait(A.at[parts[i], both, below, :, tile(u)], y_r.at[u, i, 0])
            v = A.at[parts[i], 0, below, :, tile(u)]
            send(v, v, y_s.at[u, i, 2], y_r.at[u, i, 2], ydev(1))
            wait(A.at[parts[i], both, above, :, tile(u)], y_r.at[u, i, 1])
            v = A.at[parts[i], 1, above, :, tile(u)]
            send(v, v, y_s.at[u, i, 3], y_r.at[u, i, 3], ydev(3))

    def y_done(u):
        for i in range(2):
            wait(A.at[parts[i], 0, far, :, tile(u)], y_r.at[u, i, 2])
            wait(A.at[parts[i], 1, far, :, tile(u)], y_r.at[u, i, 3])

    def y_drain(u):
        for i in range(2):
            wait(A.at[parts[i], both, y, :, tile(u)], y_s.at[u, i, 0])
            wait(A.at[parts[i], both, y, :, tile(u)], y_s.at[u, i, 1])
            wait(A.at[parts[i], 0, below, :, tile(u)], y_s.at[u, i, 2])
            wait(A.at[parts[i], 1, above, :, tile(u)], y_s.at[u, i, 3])

    q_own(0, 0)
    q_own(1, 0)
    wait(A.at[0, 1 - c, :, :, pieces[0]], pair_r.at[0])
    q_own(0, 1)
    q_own(2, 0)

    loads[2].wait()
    loads[3].wait()
    lax.fori_loop(0, 10, turn, 0)
    half = GO.at[:, of(c * TOK, TOK)]
    send(half, half, pair_s.at[2], pair_r.at[2], partner)
    wait(A.at[0, 1 - c, :, :, pieces[1]], pair_r.at[1])
    q_own(1, 1)
    q_relay(0)
    q_own(2, 1)
    q_near(0)
    y_own(0, 0)

    def block(da, p, part, n):
        aa = lax.rem(a + da, 4)
        bb = lax.rem(b + B_OFF[p], 4)
        start = (bb * 4 + aa + c * 3 * (aa - bb)) * BLK + part * OWN
        return pl.ds(pl.multiple_of(start, OWN), n)

    wait(GO.at[:, of((1 - c) * TOK, TOK)], pair_r.at[2])
    own_copies = [
        pltpu.make_async_copy(GO.at[block(0, p, 0, BLK)], G.at[p, :, pl.ds(0, 512)], own_sem.at[p])
        for p in range(4)
    ]

    def hop(p):
        send(GO.at[block(2, p, 0, OWN)], RB.at[0, p], hop_s.at[0, p], hop_r.at[0, p], gdev(1))
        send(GO.at[block(2, p, 1, OWN)], RB.at[1, p], hop_s.at[1, p], hop_r.at[1, p], gdev(3))

    slot1, slot2, slot3 = pl.ds(512, 512), pl.ds(1024, 512), pl.ds(1536, 512)
    first, second = pl.ds(0, OWN), pl.ds(OWN, OWN)

    def near(p):
        send(GO.at[block(1, p, 0, BLK)], G.at[p, :, slot2], nbr_s.at[0, p], nbr_r.at[0, p], gdev(1))
        send(GO.at[block(3, p, 0, BLK)], G.at[p, :, slot1], nbr_s.at[1, p], nbr_r.at[1, p], gdev(3))

    def hop_relay(p):
        wait(RB.at[0, p], hop_r.at[0, p])
        send(RB.at[0, p], G.at[p, first, slot3], rel_s.at[0, p], rel_r.at[0, p], gdev(1))
        wait(RB.at[1, p], hop_r.at[1, p])
        send(RB.at[1, p], G.at[p, second, slot3], rel_s.at[1, p], rel_r.at[1, p], gdev(3))

    def block_done(p):
        own_copies[p].wait()
        wait(G.at[p, :, slot2], nbr_r.at[0, p])
        wait(G.at[p, :, slot1], nbr_r.at[1, p])
        wait(G.at[p, first, slot3], rel_r.at[0, p])
        wait(G.at[p, second, slot3], rel_r.at[1, p])

    q_relay(1)
    hop(0)
    for cp in own_copies:
        cp.start()
    q_far(0)
    y_own(0, 1)
    q_near(1)
    y_own(1, 0)
    q_relay(2)
    for p in range(1, 4):
        hop(p)
    near(0)
    q_far(1)
    y_own(1, 1)
    y_relay(0)
    y_own(2, 0)
    y_own(2, 1)
    hop_relay(0)
    near(1)
    hop_relay(1)
    near(2)
    q_near(2)
    q_far(2)
    y_relay(1)
    y_own(3, 0)
    y_own(3, 1)
    hop_relay(2)
    near(3)
    hop_relay(3)
    for u in range(2, 4):
        y_relay(u)
        y_own(u + 2, 0)
        y_own(u + 2, 1)

    for p in range(3):
        block_done(p)
    acc[...] = jnp.zeros_like(acc)

    def out_tile(h, t):
        return pl.ds(pl.multiple_of(h * HALF + t * TILE, TILE), TILE)

    def product(p, n, t):
        acts = A[:, :, :, :, tile(t)].reshape(4 * 512, TILE)
        left = G[p : p + n].reshape(n * BLK, 2048)
        return jnp.dot(left, acts, preferred_element_type=F32).astype(BF).reshape(n, BLK, TILE)

    def reduce_send(d, part, core, t):
        src = PB.at[1 + d, pl.ds(part * OWN, OWN), tile(t)]
        send(src, RF.at[d, :, out_tile(c, t)], rf_s.at[d, core, t], rf_r.at[d, c, t], rdev(1 + 2 * d, core))

    def add_send(t):
        for d in (0, 1):
            wait(H.at[d, :, tile(t)], rh_r.at[d, t])
            rows = pl.ds(d * OWN, OWN)
            total = PB[1 + d, rows, tile(t)].astype(F32) + H[d, :, tile(t)].astype(F32)
            PB[1 + d, rows, tile(t)] = total.astype(BF)
            reduce_send(d, d, d, t)

    keep = of(c * OWN, OWN)
    give = of((1 - c) * OWN, OWN)

    def own_block(t):
        PB[3, :, tile(t)] = product(3, 1, t)[0]
        send(PB.at[3, give, tile(t)], PP.at[:, out_tile(c, t)], pp_s.at[t], pp_r.at[t], partner)
        PP[:, out_tile(c, t)] = PB[3, keep, tile(t)]

    def copy_out(h, t):
        cols = out_tile(h, t)
        return pltpu.make_async_copy(GR.at[:, cols], grad_out.at[:, cols], out_sem.at[h, t])

    def finish(t):
        wait(PP.at[:, out_tile(1 - c, t)], pp_r.at[t])
        for h in (0, 1):
            cols = out_tile(h, t)
            wait(RF.at[0, :, cols], rf_r.at[0, h, t])
            wait(RF.at[1, :, cols], rf_r.at[1, h, t])
            g = PP[:, cols].astype(F32) + RF[0, :, cols].astype(F32) + RF[1, :, cols].astype(F32)
            GR[:, cols] = g
            copy_out(h, t).start()
            sq = jnp.sum((g * g).reshape(OWN // 8, 8, TILE), axis=0)
            acc[...] += sq[:, :128] + sq[:, 128:]

    def step(t, _):
        y_done(t)
        PB[0:3, :, tile(t)] = product(0, 3, t)
        send(PB.at[0, first, tile(t)], H.at[0, :, tile(t)], rh_s.at[0, t], rh_r.at[0, t], rdev(1, c))
        send(PB.at[0, second, tile(t)], H.at[1, :, tile(t)], rh_s.at[1, t], rh_r.at[1, t], rdev(3, c))
        reduce_send(0, 1, 1, t)
        reduce_send(1, 0, 0, t)

        @pl.when(lax.rem(t, 2) == 0)
        def _():
            u = 4 + lax.div(t, 2)
            y_relay(u)

            @pl.when(u < STEPS - 2)
            def _():
                y_own(u + 2, 0)
                y_own(u + 2, 1)

        @pl.when(t >= 1)
        def _():
            add_send(t - 1)

        @pl.when(t == 2)
        def _():
            block_done(3)

        @pl.when(t >= 2)
        def _():
            own_block(t - 2)

        @pl.when(t >= 3)
        def _():
            finish(t - 3)

        return 0

    lax.fori_loop(0, STEPS, step, 0)
    own_block(STEPS - 2)
    own_block(STEPS - 1)
    add_send(STEPS - 1)

    def last(t, _):
        finish(t)
        return 0

    lax.fori_loop(STEPS - 3, STEPS, last, 0)

    NS[0] = acc[...]
    sent = []
    for dz in range(4):
        for dc in range(2):
            i = dz * 2 + dc
            if i:
                dev = (lax.rem(z + dz, 4), x, lax.rem(c + dc, 2), y)
                send(NS.at[0], N1.at[i - 1], n_s.at[i - 1], n_r.at[i - 1], dev)
                sent.append((0, i - 1))
    for i in range(7):
        wait(N1.at[i], n_r.at[i])
    NS[1] = NS[0] + jnp.sum(N1[...], axis=0)
    for i in range(3):
        dev = (z, lax.rem(x + i + 1, 4), c, y)
        send(NS.at[1], N2.at[i], n_s.at[7 + i], n_r.at[7 + i], dev)
        sent.append((1, 7 + i))
    for i in range(3):
        wait(N2.at[i], n_r.at[7 + i])
    NS[2] = NS[1] + jnp.sum(N2[...], axis=0)
    for i in range(3):
        send(NS.at[2], N3.at[i], n_s.at[10 + i], n_r.at[10 + i], ydev(i + 1))
        sent.append((2, 10 + i))

    for i in range(2):
        wait(S.at[:, :, pieces[i]], pair_s.at[i])
    wait(half, pair_s.at[2])
    for g in range(3):
        q_drain(g)
    for p in range(4):
        for d in (0, 1):
            wait(RB.at[d, p], hop_s.at[d, p])
            wait(RB.at[d, p], rel_s.at[d, p])
            wait(G.at[p, :, slot1], nbr_s.at[d, p])

    def drain(t, _):
        y_drain(t)
        for d in (0, 1):
            wait(H.at[d, :, tile(t)], rh_s.at[d, t])
            for core in (0, 1):
                wait(H.at[d, :, tile(t)], rf_s.at[d, core, t])
            copy_out(d, t).wait()
        wait(H.at[0, :, tile(t)], pp_s.at[t])
        return 0

    lax.fori_loop(0, STEPS, drain, 0)
    for i in range(3):
        wait(N3.at[i], n_r.at[10 + i])
    total = jnp.sum(NS[2] + jnp.sum(N3[...], axis=0), keepdims=True)
    limit = clip_rms * jnp.sqrt(jnp.full((1, 1), FF * ROWS, F32))
    factor_out[...] = jnp.minimum(1.0, limit / jnp.sqrt(total))
    for i, k in sent:
        wait(NS.at[i], n_s.at[k])


def owned_gradient(activations, out_grads, act_scale, grad_scale):
    dma = pltpu.SemaphoreType.DMA
    vmem = pltpu.VMEM
    scratch = [
        vmem((2, 128, ROWS), BF),
        vmem((2, 128, 5120), BF),
        vmem((2, ROWS // 128), BF),
        vmem((2, 5120), BF),
        vmem((2, ROWS), F32),
        vmem((4, 2, 4, 64, HALF), BF),
        vmem((4, 64, HALF), BF),
        vmem((5120, 512), BF),
        vmem((4, BLK, 2048), BF),
        vmem((2, 4, OWN, 512), BF),
        vmem((4, BLK, HALF), BF),
        vmem((2, OWN, HALF), BF),
        vmem((2, OWN, ROWS), BF),
        vmem((OWN, ROWS), BF),
        vmem((OWN, ROWS), F32),
        vmem((8, 128), F32),
        vmem((3, 8, 128), F32),
        vmem((7, 8, 128), F32),
        vmem((3, 8, 128), F32),
        vmem((3, 8, 128), F32),
        dma((4,)),
        dma((4,)),
        dma((3,)), dma((3,)),
        dma((3, 3, 2)), dma((3, 3, 2)),
        dma((STEPS, 2, 4)), dma((STEPS, 2, 4)),
        dma((2, 4)), dma((2, 4)),
        dma((2, 4)), dma((2, 4)),
        dma((2, 4)), dma((2, 4)),
        dma((2, STEPS)), dma((2, STEPS)),
        dma((2, 2, STEPS)), dma((2, 2, STEPS)),
        dma((STEPS,)), dma((STEPS,)),
        dma((2, STEPS)),
        dma((13,)), dma((13,)),
    ]
    return pl.pallas_call(
        kernel,
        out_shape=(
            jax.ShapeDtypeStruct((OWN, ROWS), F32),
            jax.ShapeDtypeStruct((1, 1), F32),
        ),
        in_specs=[pl.BlockSpec(memory_space=pltpu.HBM)] * 4,
        out_specs=(pl.BlockSpec(memory_space=pl.ANY), pl.BlockSpec(memory_space=vmem)),
        scratch_shapes=scratch,
        compiler_params=pltpu.CompilerParams(
            collective_id=0, has_side_effects=True, vmem_limit_bytes=46 * 1024 * 1024
        ),
        cost_estimate=pl.CostEstimate(
            flops=2 * 8192 * OWN * ROWS, bytes_accessed=8 * 1024 * 1024, transcendentals=0
        ),
        name="owned_gradient",
    )(*(
        pltpu.with_memory_space_constraint(v, pltpu.HBM)
        for v in (activations, out_grads, act_scale, grad_scale.reshape(2, 5120))
    ))


def per_device(activations, out_grads, act_scale, grad_scale, moment, second, master):
    grad_owned, factors = owned_gradient(activations, out_grads, act_scale, grad_scale)
    clipped = factors.reshape(()) * grad_owned
    new_moment = beta_first * moment + (1.0 - beta_first) * clipped
    new_second = beta_second * second + (1.0 - beta_second) * clipped * clipped
    new_master = master - learn_rate * new_moment / (jnp.sqrt(new_second) + adam_eps)
    weights = new_master.astype(jnp.bfloat16)
    return (new_moment, new_second, new_master, weights)


def solution(mesh):
    finer = Mesh(
        mesh.devices.reshape(4, 4, 2, mesh.shape["tensor"]), ("dp_0", "dp_1", "dp_2", "tensor")
    )
    in_specs = (
        P(DP, None, None),
        P(DP, None, "tensor"),
        P(DP, None),
        P(DP, None, "tensor"),
        P(TENSOR_DP, None),
        P(TENSOR_DP, None),
        P(TENSOR_DP, None),
    )
    out_specs = (P(TENSOR_DP, None), P(TENSOR_DP, None), P(TENSOR_DP, None), P(TENSOR_DP, None))
    return jax.shard_map(
        per_device, mesh=finer, in_specs=in_specs, out_specs=out_specs, check_vma=False
    )
```

```python
import functools

import jax
import jax.numpy as jnp
from jax import lax
from jax.experimental import pallas as pl
from jax.experimental.pallas import tpu as pltpu
from jax.sharding import Mesh
from jax.sharding import PartitionSpec as P

FF = 20480
ROWS = 4096
DP = ("dp_0", "dp_1", "dp_2")
TENSOR_DP = ("tensor", "dp_0", "dp_1", "dp_2")

clip_rms = 1.0
beta_first = 0.9
beta_second = 0.95
learn_rate = 0.003
adam_eps = 1e-08

TOK = 256
HALF = ROWS // 2
TILE = 256
STEPS = HALF // TILE
BLK = 320
OWN = 160
QUART = 128
B_OFF = (2, 1, 3, 0)
BF = jnp.bfloat16
F32 = jnp.float32


def kernel(
    acts_hbm, grads_hbm, ascale_hbm, gscale_hbm,
    grad_out, factor_out,
    acts_raw, grads_raw, ascale, gscale, wide, A, S, GO, G, RB, PB, H, RF, PP, GR, acc, NS, N1,
    load_sem, own_sem, pair_s, pair_r, q_s, q_r, y_s, y_r,
    hop_s, hop_r, nbr_s, rel_s, blk_r,
    rh_s, rh_r, rf_s, pp_s, fin_r, out_sem, n_s, n_r,
):
    z = lax.axis_index("dp_0")
    x = lax.axis_index("dp_1")
    c = lax.axis_index("dp_2")
    y = lax.axis_index("tensor")
    a = x + c * (z - x)
    b = z + c * (x - z)

    def gdev(d):
        return (lax.rem(z + c * d, 4), lax.rem(x + (1 - c) * d, 4), c, y)

    def rdev(d, core):
        return (lax.rem(z + (1 - c) * d, 4), lax.rem(x + c * d, 4), core, y)

    def ydev(d):
        return (z, x, c, lax.rem(y + d, 4))

    partner = (z, x, 1 - c, y)
    MESH = pl.DeviceIdType.MESH

    def send(src, dst, ss, rs, dev):
        pltpu.make_async_remote_copy(
            src_ref=src, dst_ref=dst, send_sem=ss, recv_sem=rs, device_id=dev, device_id_type=MESH
        ).start()

    def wait(ref, sem):
        pltpu.make_async_copy(ref, ref, sem).wait()

    def of(i, n):
        return pl.ds(pl.multiple_of(i, n), n)

    barrier = pltpu.get_barrier_semaphore()
    greet = [partner]
    for d in (1, 3):
        for core in (0, 1):
            greet.append((lax.rem(z + d, 4), x, core, y))
            greet.append((z, lax.rem(x + d, 4), core, y))
        greet.append(ydev(d))
    for dev in greet:
        pl.semaphore_signal(barrier, inc=1, device_id=dev, device_id_type=MESH)
    loads = [
        pltpu.make_async_copy(src, dst, load_sem.at[i])
        for i, (src, dst) in enumerate(
            ((ascale_hbm, ascale), (acts_hbm, acts_raw), (gscale_hbm, gscale), (grads_hbm, grads_raw))
        )
    ]
    for load in loads:
        load.start()

    loads[0].wait()
    for r in range(ROWS // 128):
        wide[:, r * 128 : (r + 1) * 128] = jnp.broadcast_to(
            ascale[:, r : r + 1].astype(F32), (2, 128)
        )
    loads[1].wait()

    def scale_step(i, _):
        dst = pl.ds(pl.multiple_of(i * 512, 512), 512)
        for which, put in ((1 - c, 0), (c, 1)):
            cols = pl.ds(pl.multiple_of(which * HALF + i * 512, 512), 512)
            for blk in range(2):
                v = (acts_raw[blk, :, cols].astype(F32) * wide[blk : blk + 1, cols]).astype(BF)
                v = v.reshape(2, 64, 512)
                rows = pl.ds(2 * blk, 2)
                if put:
                    A[0, c, rows, :, dst] = v
                else:
                    S[rows, :, dst] = v
        return 0

    lax.fori_loop(0, HALF // 512, scale_step, 0)

    def turn(i, _):
        cols = pl.ds(pl.multiple_of(i * 512, 512), 512)
        for blk in range(2):
            v = grads_raw[blk, :, cols].astype(F32) * gscale[blk : blk + 1, cols].astype(F32)
            GO[cols, of(c * TOK + blk * 128, 128)] = v.T.astype(BF)
        return 0

    pl.semaphore_wait(barrier, len(greet))

    far = lax.rem(y + 2, 4)
    last_tile = pl.ds(HALF - TILE, TILE)
    groups = (
        (pl.ds(0, TILE), y),
        (pl.ds(TILE, 2 * TILE), y),
        (pl.ds(3 * TILE, HALF - 3 * TILE), y),
        (last_tile, far),
    )
    pieces = (pl.ds(0, TILE), pl.ds(TILE, HALF - TILE))
    def q_own(g, k):
        cols, q = groups[g]
        e = 3 * (g // 3)
        who = c + k * (1 - 2 * c)
        src = A.at[0, who, q, :, cols]
        send(src, A.at[2, who, q, :, cols], q_s.at[e, k], q_r.at[g, 0, who], gdev(1))
        send(src, A.at[1, who, q, :, cols], q_s.at[e + 1, k], q_r.at[g, 1, who], gdev(3))

    def first_group():
        cols, q = groups[0]
        q_own(0, 0)
        src = S.at[q, :, cols]
        send(src, A.at[2, c, q, :, cols], q_s.at[0, 1], q_r.at[0, 0, c], rdev(1, 1 - c))
        send(src, A.at[1, c, q, :, cols], q_s.at[1, 1], q_r.at[0, 1, c], rdev(3, 1 - c))

    def q_relay(g):
        cols, q = groups[g]
        e = 3 * (g // 3) + 2
        wait(A.at[2, 0, q, :, cols], q_r.at[g, 0, 0])
        send(A.at[2, 0, q, :, cols], A.at[3, 0, q, :, cols], q_s.at[e, 0], q_r.at[g, 2, 0], gdev(1))
        wait(A.at[1, 1, q, :, cols], q_r.at[g, 1, 1])
        send(A.at[1, 1, q, :, cols], A.at[3, 1, q, :, cols], q_s.at[e, 1], q_r.at[g, 2, 1], gdev(3))

    def q_near(g):
        cols, q = groups[g]
        wait(A.at[2, 1, q, :, cols], q_r.at[g, 0, 1])
        wait(A.at[1, 0, q, :, cols], q_r.at[g, 1, 0])

    def q_far(g):
        cols, q = groups[g]
        wait(A.at[3, 0, q, :, cols], q_r.at[g, 2, 0])
        wait(A.at[3, 1, q, :, cols], q_r.at[g, 2, 1])

    def q_drain():
        for i in range(3):
            for k in range(2):
                wait(A.at[0, 0, y], q_s.at[i, k])
                wait(A.at[0, 0, y, :, last_tile], q_s.at[3 + i, k])

    def tile(t):
        return pl.ds(pl.multiple_of(t * TILE, TILE), TILE)

    parts = (pl.ds(1, 2), pl.ds(3, 1))
    both = pl.ds(0, 2)
    below = lax.rem(y + 3, 4)
    above = lax.rem(y + 1, 4)

    def y_own(u, i):
        v = A.at[parts[i], both, y, :, tile(u)]
        send(v, v, y_s.at[i, 0], y_r.at[u, 0], ydev(1))
        send(v, v, y_s.at[i, 1], y_r.at[u, 1], ydev(3))

    three = pl.ds(1, 3)

    def y_relay(u):
        wait(A.at[three, both, below, :, tile(u)], y_r.at[u, 0])
        v = A.at[three, 0, below, :, tile(u)]
        send(v, v, y_s.at[2, 0], y_r.at[u, 2], ydev(1))
        wait(A.at[three, both, above, :, tile(u)], y_r.at[u, 1])
        v = A.at[three, 1, above, :, tile(u)]
        send(v, v, y_s.at[2, 1], y_r.at[u, 2], ydev(3))

    def y_done(u):
        wait(A.at[three, both, far, :, tile(u)], y_r.at[u, 2])

    def y_drain():
        for k in range(2):
            for i in range(2):
                wait(A.at[parts[i], both, y], y_s.at[i, k])
            wait(A.at[three, 0, y, :, pl.ds(0, HALF - TILE)], y_s.at[2, k])

    def y_near(u):
        wait(A.at[three, both, below, :, tile(u)], y_r.at[u, 0])
        wait(A.at[three, both, above, :, tile(u)], y_r.at[u, 1])

    first_group()
    for i in range(2):
        send(S.at[:, :, pieces[i]], A.at[0, c, :, :, pieces[i]], pair_s.at[i], pair_r.at[i], partner)
    q_own(1, 0)
    q_own(2, 0)
    wait(A.at[0, 1 - c, :, :, pieces[0]], pair_r.at[0])

    loads[2].wait()
    loads[3].wait()
    lax.fori_loop(0, 10, turn, 0)
    half = GO.at[:, of(c * TOK, TOK)]
    send(half, half, pair_s.at[2], pair_r.at[2], partner)
    wait(A.at[0, 1 - c, :, :, pieces[1]], pair_r.at[1])
    q_own(1, 1)
    q_own(2, 1)
    q_relay(0)
    q_near(0)
    y_own(0, 0)
    q_relay(1)

    def block(da, p, part, n):
        aa = lax.rem(a + da, 4)
        bb = lax.rem(b + B_OFF[p], 4)
        start = (bb * 4 + aa + c * 3 * (aa - bb)) * BLK + part * OWN
        return pl.ds(pl.multiple_of(start, OWN), n)

    wait(GO.at[:, of((1 - c) * TOK, TOK)], pair_r.at[2])
    own_copies = [
        pltpu.make_async_copy(GO.at[block(0, p, 0, BLK)], G.at[p, :, pl.ds(0, 512)], own_sem.at[p])
        for p in range(4)
    ]

    def hop(p):
        send(GO.at[block(2, p, 0, OWN)], RB.at[0, p], hop_s.at[0], hop_r.at[0, p], gdev(1))
        send(GO.at[block(2, p, 1, OWN)], RB.at[1, p], hop_s.at[1], hop_r.at[1, p], gdev(3))

    slot1, slot2, slot3 = pl.ds(512, 512), pl.ds(1024, 512), pl.ds(1536, 512)
    first, second = pl.ds(0, OWN), pl.ds(OWN, OWN)

    def near(p):
        send(GO.at[block(1, p, 0, BLK)], G.at[p, :, slot2], nbr_s.at[0], blk_r.at[p], gdev(1))
        send(GO.at[block(3, p, 0, BLK)], G.at[p, :, slot1], nbr_s.at[1], blk_r.at[p], gdev(3))

    def hop_relay(p):
        wait(RB.at[0, p], hop_r.at[0, p])
        send(RB.at[0, p], G.at[p, first, slot3], rel_s.at[0], blk_r.at[p], gdev(1))
        wait(RB.at[1, p], hop_r.at[1, p])
        send(RB.at[1, p], G.at[p, second, slot3], rel_s.at[1], blk_r.at[p], gdev(3))

    def block_done(p):
        own_copies[p].wait()
        wait(G.at[p, :, pl.ds(512, 1536)], blk_r.at[p])

    hop(0)
    q_near(1)
    y_own(1, 0)
    q_far(0)
    y_own(0, 1)
    for cp in own_copies:
        cp.start()
    q_far(1)
    y_own(1, 1)
    q_relay(2)
    for p in range(1, 4):
        hop(p)
    near(0)

    def y_both(u):
        y_own(u, 0)
        y_own(u, 1)

    y_both(2)
    y_relay(0)
    q_near(2)
    q_far(2)
    y_both(3)
    hop_relay(0)
    near(1)
    hop_relay(1)
    near(2)
    y_relay(1)
    hop_relay(2)
    near(3)
    hop_relay(3)
    q_own(3, 0)
    q_own(3, 1)
    y_relay(2)
    y_both(4)
    y_relay(3)
    y_both(5)
    y_relay(4)
    y_both(6)

    for p in range(3):
        block_done(p)
    acc[...] = jnp.zeros_like(acc)

    def out_tile(h, t):
        return pl.ds(pl.multiple_of(h * HALF + t * TILE, TILE), TILE)

    def product(p, n, t):
        acts = A[:, :, :, :, tile(t)].reshape(4 * 512, TILE)
        left = G[p : p + n].reshape(n * BLK, 2048)
        return jnp.dot(left, acts, preferred_element_type=F32).astype(BF).reshape(n, BLK, TILE)

    def reduce_send(d, part, core, t):
        src = PB.at[1 + d, pl.ds(part * OWN, OWN), tile(t)]
        send(src, RF.at[d, :, out_tile(c, t)], rf_s.at[d, core], fin_r.at[t], rdev(1 + 2 * d, core))

    def add_send(t):
        for d in (0, 1):
            wait(H.at[d, :, tile(t)], rh_r.at[d, t])
            rows = pl.ds(d * OWN, OWN)
            total = PB[1 + d, rows, tile(t)].astype(F32) + H[d, :, tile(t)].astype(F32)
            PB[1 + d, rows, tile(t)] = total.astype(BF)
            reduce_send(d, d, d, t)

    keep = of(c * OWN, OWN)
    give = of((1 - c) * OWN, OWN)

    def own_block(t):
        PB[3, :, tile(t)] = product(3, 1, t)[0]
        send(PB.at[3, give, tile(t)], PP.at[:, out_tile(c, t)], pp_s.at[0], fin_r.at[t], partner)
        PP[:, out_tile(c, t)] = PB[3, keep, tile(t)]

    def copy_out(h, t):
        cols = out_tile(h, t)
        return pltpu.make_async_copy(GR.at[:, cols], grad_out.at[:, cols], out_sem.at[0])

    def finish(t):
        wait(RF.at[0, :, pl.ds(0, 5 * TILE)], fin_r.at[t])
        for h in (0, 1):
            cols = out_tile(h, t)
            g = PP[:, cols].astype(F32) + RF[0, :, cols].astype(F32) + RF[1, :, cols].astype(F32)
            GR[:, cols] = g
            copy_out(h, t).start()
            sq = jnp.sum((g * g).reshape(OWN // 8, 8, TILE), axis=0)
            acc[...] += sq[:, :128] + sq[:, 128:]

    def relay_and_send(u):
        y_relay(u)
        if u + 2 < STEPS:
            y_both(u + 2)

    def last_arrivals():
        q_near(3)
        q_far(3)
        y_near(STEPS - 1)

    def step(t, _):
        pl.when(t < STEPS - 1)(functools.partial(y_done, t))
        pl.when(t == STEPS - 1)(last_arrivals)
        PB[0:3, :, tile(t)] = product(0, 3, t)
        send(PB.at[0, first, tile(t)], H.at[0, :, tile(t)], rh_s.at[0], rh_r.at[0, t], rdev(1, c))
        send(PB.at[0, second, tile(t)], H.at[1, :, tile(t)], rh_s.at[1], rh_r.at[1, t], rdev(3, c))
        reduce_send(0, 1, 1, t)
        reduce_send(1, 0, 0, t)

        for at, u in ((1, 5), (3, 6)):
            pl.when(t == at)(functools.partial(relay_and_send, u))
        pl.when(t == 3)(functools.partial(q_relay, 3))

        pl.when(t >= 1)(functools.partial(add_send, t - 1))
        pl.when(t == 2)(functools.partial(block_done, 3))
        pl.when(t == 2)(functools.partial(own_block, t - 2))
        pl.when(t == 3)(functools.partial(own_block, t - 2))
        pl.when(t >= 3)(functools.partial(own_block, t - 1))
        pl.when(t >= 3)(functools.partial(finish, t - 3))
        return 0

    lax.fori_loop(0, STEPS, step, 0)
    own_block(STEPS - 1)
    add_send(STEPS - 1)

    def last(t, _):
        finish(t)
        return 0

    lax.fori_loop(STEPS - 3, STEPS, last, 0)

    me = ((z * 4 + x) * 2 + c) * 4 + y
    NS[0] = jnp.sum(acc[...], axis=0, keepdims=True)
    N1[me] = NS[0]

    def tell(dz, far, i, _):
        dev = (
            lax.rem(z + dz, 4),
            lax.rem(x + far + lax.div(i, 8), 4),
            lax.rem(c + lax.rem(lax.div(i, 4), 2), 2),
            lax.rem(y + far + lax.rem(i, 4), 4),
        )
        send(NS.at[0], N1.at[me], n_s.at[0], n_r.at[0], dev)
        return 0

    for dz in (2, 1, 3):
        lax.fori_loop(0, 32, functools.partial(tell, dz, 2), 0)
    lax.fori_loop(1, 32, functools.partial(tell, 0, 0), 0)

    for i in range(2):
        wait(S.at[:, :, pieces[i]], pair_s.at[i])
    wait(half, pair_s.at[2])
    q_drain()
    for d in (0, 1):
        wait(RB.at[d], hop_s.at[d])
        wait(RB.at[d], rel_s.at[d])
        wait(G.at[:, :, slot1], nbr_s.at[d])
        wait(H.at[d], rh_s.at[d])
        for core in (0, 1):
            wait(H.at[d], rf_s.at[d, core])
    wait(H.at[0], pp_s.at[0])
    wait(GR, out_sem.at[0])
    y_drain()
    others = N1.at[pl.ds(0, 127)]
    wait(others, n_r.at[0])
    total = jnp.sum(jnp.sum(N1[...], axis=0), keepdims=True)
    limit = clip_rms * jnp.sqrt(jnp.full((1, 1), FF * ROWS, F32))
    factor_out[...] = jnp.broadcast_to(jnp.minimum(1.0, limit / jnp.sqrt(total)), (8, 128))
    wait(others, n_s.at[0])


def adam_kernel(factor, grad, moment, second, master, nm_out, ns_out, nw_out, w_out, nm, ns, nw, w, sems):
    f = factor[0:1, 0:1]
    pairs = ((nm, nm_out), (ns, ns_out), (nw, nw_out), (w, w_out))

    def step(i, _):
        rows = pl.ds(pl.multiple_of(i * 16, 16), 16)
        clipped = f * grad[rows, :]
        new_moment = beta_first * moment[rows, :] + (1.0 - beta_first) * clipped
        new_second = beta_second * second[rows, :] + (1.0 - beta_second) * clipped * clipped
        new_master = master[rows, :] - learn_rate * new_moment / (jnp.sqrt(new_second) + adam_eps)
        nm[rows, :] = new_moment
        ns[rows, :] = new_second
        nw[rows, :] = new_master
        w[rows, :] = new_master.astype(BF)
        for k, (src, dst) in enumerate(pairs):
            pltpu.make_async_copy(src.at[rows], dst.at[rows], sems.at[k]).start()
        return 0

    lax.fori_loop(0, OWN // 16, step, 0)
    for k, (src, dst) in enumerate(pairs):
        pltpu.make_async_copy(src, dst, sems.at[k]).wait()


def adam(factor, grad, moment, second, master):
    vmem = pltpu.VMEM
    shape = (OWN, ROWS)
    kinds = (F32, F32, F32, BF)
    return pl.pallas_call(
        adam_kernel,
        out_shape=tuple(jax.ShapeDtypeStruct(shape, kind) for kind in kinds),
        in_specs=[pl.BlockSpec(memory_space=vmem)] * 5,
        out_specs=tuple(pl.BlockSpec(memory_space=pltpu.HBM) for _ in kinds),
        scratch_shapes=[vmem(shape, kind) for kind in kinds] + [pltpu.SemaphoreType.DMA((4,))],
        compiler_params=pltpu.CompilerParams(vmem_limit_bytes=24 * 1024 * 1024),
        cost_estimate=pl.CostEstimate(flops=20 * OWN * ROWS, bytes_accessed=30 * OWN * ROWS, transcendentals=OWN * ROWS),
        name="adam",
    )(factor, grad, moment, second, master)


def owned_gradient(activations, out_grads, act_scale, grad_scale):
    dma = pltpu.SemaphoreType.DMA
    vmem = pltpu.VMEM
    scratch = [
        vmem((2, 128, ROWS), BF),
        vmem((2, 128, 5120), BF),
        vmem((2, ROWS // 128), BF),
        vmem((2, 5120), BF),
        vmem((2, ROWS), F32),
        vmem((4, 2, 4, 64, HALF), BF),
        vmem((4, 64, HALF), BF),
        vmem((5120, 512), BF),
        vmem((4, BLK, 2048), BF),
        vmem((2, 4, OWN, 512), BF),
        vmem((4, BLK, HALF), BF),
        vmem((2, OWN, HALF), BF),
        vmem((2, OWN, ROWS), BF),
        vmem((OWN, ROWS), BF),
        vmem((OWN, ROWS), F32),
        vmem((8, 128), F32),
        vmem((1, 1, 128), F32),
        vmem((128, 1, 128), F32),
        dma((4,)),
        dma((4,)),
        dma((3,)), dma((3,)),
        dma((6, 2)), dma((4, 3, 2)),
        dma((3, 2)), dma((STEPS, 3)),
        dma((2,)), dma((2, 4)),
        dma((2,)), dma((2,)), dma((4,)),
        dma((2,)), dma((2, STEPS)),
        dma((2, 2)), dma((1,)), dma((STEPS,)),
        dma((1,)),
        dma((1,)), dma((1,)),
    ]
    return pl.pallas_call(
        kernel,
        out_shape=(
            jax.ShapeDtypeStruct((OWN, ROWS), F32),
            jax.ShapeDtypeStruct((8, 128), F32),
        ),
        in_specs=[pl.BlockSpec(memory_space=pltpu.HBM)] * 4,
        out_specs=(pl.BlockSpec(memory_space=pl.ANY), pl.BlockSpec(memory_space=vmem)),
        scratch_shapes=scratch,
        compiler_params=pltpu.CompilerParams(
            collective_id=0, has_side_effects=True, vmem_limit_bytes=46 * 1024 * 1024
        ),
        cost_estimate=pl.CostEstimate(
            flops=2 * 8192 * OWN * ROWS, bytes_accessed=8 * 1024 * 1024, transcendentals=0
        ),
        name="owned_gradient",
    )(*(
        pltpu.with_memory_space_constraint(v, pltpu.HBM)
        for v in (activations, out_grads, act_scale, grad_scale.reshape(2, 5120))
    ))


def per_device(activations, out_grads, act_scale, grad_scale, moment, second, master):
    grad_owned, factors = owned_gradient(activations, out_grads, act_scale, grad_scale)
    return adam(factors, grad_owned, moment, second, master)


def solution(mesh):
    finer = Mesh(
        mesh.devices.reshape(4, 4, 2, mesh.shape["tensor"]), ("dp_0", "dp_1", "dp_2", "tensor")
    )
    in_specs = (
        P(DP, None, None),
        P(DP, None, "tensor"),
        P(DP, None),
        P(DP, None, "tensor"),
        P(TENSOR_DP, None),
        P(TENSOR_DP, None),
        P(TENSOR_DP, None),
    )
    out_specs = (P(TENSOR_DP, None), P(TENSOR_DP, None), P(TENSOR_DP, None), P(TENSOR_DP, None))
    return jax.shard_map(
        per_device, mesh=finer, in_specs=in_specs, out_specs=out_specs, check_vma=False
    )
```

```python
import functools

import jax
import jax.numpy as jnp
from jax import lax
from jax.experimental import pallas as pl
from jax.experimental.pallas import tpu as pltpu
from jax.sharding import Mesh
from jax.sharding import PartitionSpec as P

FF = 20480
ROWS = 4096
DP = ("dp_0", "dp_1", "dp_2")
TENSOR_DP = ("tensor", "dp_0", "dp_1", "dp_2")

clip_rms = 1.0
beta_first = 0.9
beta_second = 0.95
learn_rate = 0.003
adam_eps = 1e-08

TOK = 256
HALF = ROWS // 2
TILE = 256
STEPS = HALF // TILE
BLK = 320
OWN = 160
QUART = 128
B_OFF = (2, 1, 3, 0)
BF = jnp.bfloat16
F32 = jnp.float32


def kernel(
    acts_hbm, grads_hbm, ascale_hbm, gscale_hbm,
    grad_out, factor_out,
    acts_raw, grads_raw, ascale, gscale, wide, A, S, GO, G, RB, PB, H, RF, PP, GR, acc, NS, N1,
    load_sem, own_sem, pair_s, pair_r, q_s, q_r, y_s, y_r,
    hop_s, hop_r, nbr_s, rel_s, blk_r,
    rh_s, rh_r, rf_s, pp_s, fin_r, out_sem, n_s, n_r,
):
    z = lax.axis_index("dp_0")
    x = lax.axis_index("dp_1")
    c = lax.axis_index("dp_2")
    y = lax.axis_index("tensor")
    a = x + c * (z - x)
    b = z + c * (x - z)

    def gdev(d):
        return (lax.rem(z + c * d, 4), lax.rem(x + (1 - c) * d, 4), c, y)

    def rdev(d, core):
        return (lax.rem(z + (1 - c) * d, 4), lax.rem(x + c * d, 4), core, y)

    def ydev(d):
        return (z, x, c, lax.rem(y + d, 4))

    partner = (z, x, 1 - c, y)
    MESH = pl.DeviceIdType.MESH

    def send(src, dst, ss, rs, dev):
        pltpu.make_async_remote_copy(
            src_ref=src, dst_ref=dst, send_sem=ss, recv_sem=rs, device_id=dev, device_id_type=MESH
        ).start()

    def wait(ref, sem):
        pltpu.make_async_copy(ref, ref, sem).wait()

    def of(i, n):
        return pl.ds(pl.multiple_of(i, n), n)

    barrier = pltpu.get_barrier_semaphore()
    greet = [partner]
    for d in (1, 3):
        for core in (0, 1):
            greet.append((lax.rem(z + d, 4), x, core, y))
            greet.append((z, lax.rem(x + d, 4), core, y))
        greet.append(ydev(d))
    for dev in greet:
        pl.semaphore_signal(barrier, inc=1, device_id=dev, device_id_type=MESH)
    loads = [
        pltpu.make_async_copy(src, dst, load_sem.at[i])
        for i, (src, dst) in enumerate(
            ((ascale_hbm, ascale), (acts_hbm, acts_raw), (gscale_hbm, gscale), (grads_hbm, grads_raw))
        )
    ]
    for load in loads:
        load.start()

    loads[0].wait()
    for r in range(ROWS // 128):
        wide[:, r * 128 : (r + 1) * 128] = jnp.broadcast_to(
            ascale[:, r : r + 1].astype(F32), (2, 128)
        )
    loads[1].wait()

    def scale_step(i, _):
        dst = pl.ds(pl.multiple_of(i * 512, 512), 512)
        for which, put in ((1 - c, 0), (c, 1)):
            cols = pl.ds(pl.multiple_of(which * HALF + i * 512, 512), 512)
            for blk in range(2):
                v = (acts_raw[blk, :, cols].astype(F32) * wide[blk : blk + 1, cols]).astype(BF)
                v = v.reshape(2, 64, 512)
                rows = pl.ds(2 * blk, 2)
                if put:
                    A[0, c, rows, :, dst] = v
                else:
                    S[rows, :, dst] = v
        return 0

    lax.fori_loop(0, HALF // 512, scale_step, 0)

    def turn(i, _):
        cols = pl.ds(pl.multiple_of(i * 512, 512), 512)
        for blk in range(2):
            v = grads_raw[blk, :, cols].astype(F32) * gscale[blk : blk + 1, cols].astype(F32)
            GO[cols, of(c * TOK + blk * 128, 128)] = v.T.astype(BF)
        return 0

    pl.semaphore_wait(barrier, len(greet))

    far = lax.rem(y + 2, 4)
    last_tiles = pl.ds(HALF - 2 * TILE, 2 * TILE)
    groups = (
        (pl.ds(0, TILE), y),
        (pl.ds(TILE, 2 * TILE), y),
        (pl.ds(3 * TILE, HALF - 3 * TILE), y),
        (last_tiles, far),
    )
    pieces = (pl.ds(0, TILE), pl.ds(TILE, HALF - TILE))
    def q_own(g, k):
        cols, q = groups[g]
        e = 3 * (g // 3)
        who = c + k * (1 - 2 * c)
        src = A.at[0, who, q, :, cols]
        send(src, A.at[2, who, q, :, cols], q_s.at[e, k], q_r.at[g, 0, who], gdev(1))
        send(src, A.at[1, who, q, :, cols], q_s.at[e + 1, k], q_r.at[g, 1, who], gdev(3))

    def first_group():
        cols, q = groups[0]
        q_own(0, 0)
        src = S.at[q, :, cols]
        send(src, A.at[2, c, q, :, cols], q_s.at[0, 1], q_r.at[0, 0, c], rdev(1, 1 - c))
        send(src, A.at[1, c, q, :, cols], q_s.at[1, 1], q_r.at[0, 1, c], rdev(3, 1 - c))

    def q_relay(g):
        cols, q = groups[g]
        e = 3 * (g // 3) + 2
        wait(A.at[2, 0, q, :, cols], q_r.at[g, 0, 0])
        send(A.at[2, 0, q, :, cols], A.at[3, 0, q, :, cols], q_s.at[e, 0], q_r.at[g, 2, 0], gdev(1))
        wait(A.at[1, 1, q, :, cols], q_r.at[g, 1, 1])
        send(A.at[1, 1, q, :, cols], A.at[3, 1, q, :, cols], q_s.at[e, 1], q_r.at[g, 2, 1], gdev(3))

    def q_near(g):
        cols, q = groups[g]
        wait(A.at[2, 1, q, :, cols], q_r.at[g, 0, 1])
        wait(A.at[1, 0, q, :, cols], q_r.at[g, 1, 0])

    def q_far(g):
        cols, q = groups[g]
        wait(A.at[3, 0, q, :, cols], q_r.at[g, 2, 0])
        wait(A.at[3, 1, q, :, cols], q_r.at[g, 2, 1])

    def q_drain():
        for i in range(3):
            for k in range(2):
                wait(A.at[0, 0, y], q_s.at[i, k])
                wait(A.at[0, 0, y, :, last_tiles], q_s.at[3 + i, k])

    def tile(t):
        return pl.ds(pl.multiple_of(t * TILE, TILE), TILE)

    parts = (pl.ds(1, 2), pl.ds(3, 1))
    both = pl.ds(0, 2)
    below = lax.rem(y + 3, 4)
    above = lax.rem(y + 1, 4)

    def y_own(u, i):
        v = A.at[parts[i], both, y, :, tile(u)]
        send(v, v, y_s.at[i, 0], y_r.at[u, 0], ydev(1))
        send(v, v, y_s.at[i, 1], y_r.at[u, 1], ydev(3))

    three = pl.ds(1, 3)

    def y_relay(u):
        wait(A.at[three, both, below, :, tile(u)], y_r.at[u, 0])
        v = A.at[three, 0, below, :, tile(u)]
        send(v, v, y_s.at[2, 0], y_r.at[u, 2], ydev(1))
        wait(A.at[three, both, above, :, tile(u)], y_r.at[u, 1])
        v = A.at[three, 1, above, :, tile(u)]
        send(v, v, y_s.at[2, 1], y_r.at[u, 2], ydev(3))

    def y_done(u):
        wait(A.at[three, both, far, :, tile(u)], y_r.at[u, 2])

    def y_drain():
        for k in range(2):
            for i in range(2):
                wait(A.at[parts[i], both, y], y_s.at[i, k])
            wait(A.at[three, 0, y, :, pl.ds(0, HALF - 2 * TILE)], y_s.at[2, k])

    def y_near(u):
        wait(A.at[three, both, below, :, tile(u)], y_r.at[u, 0])
        wait(A.at[three, both, above, :, tile(u)], y_r.at[u, 1])

    first_group()
    for i in range(2):
        send(S.at[:, :, pieces[i]], A.at[0, c, :, :, pieces[i]], pair_s.at[i], pair_r.at[i], partner)
    q_own(1, 0)
    q_own(2, 0)
    wait(A.at[0, 1 - c, :, :, pieces[0]], pair_r.at[0])

    loads[2].wait()
    loads[3].wait()
    lax.fori_loop(0, 10, turn, 0)
    half = GO.at[:, of(c * TOK, TOK)]
    send(half, half, pair_s.at[2], pair_r.at[2], partner)
    wait(A.at[0, 1 - c, :, :, pieces[1]], pair_r.at[1])
    q_own(1, 1)
    q_own(2, 1)
    q_relay(0)
    q_near(0)
    y_own(0, 0)
    q_relay(1)

    def block(da, p, part, n):
        aa = lax.rem(a + da, 4)
        bb = lax.rem(b + B_OFF[p], 4)
        start = (bb * 4 + aa + c * 3 * (aa - bb)) * BLK + part * OWN
        return pl.ds(pl.multiple_of(start, OWN), n)

    wait(GO.at[:, of((1 - c) * TOK, TOK)], pair_r.at[2])
    own_copies = [
        pltpu.make_async_copy(GO.at[block(0, p, 0, BLK)], G.at[p, :, pl.ds(0, 512)], own_sem.at[p])
        for p in range(4)
    ]

    def hop(p):
        send(GO.at[block(2, p, 0, OWN)], RB.at[0, p], hop_s.at[0], hop_r.at[0, p], gdev(1))
        send(GO.at[block(2, p, 1, OWN)], RB.at[1, p], hop_s.at[1], hop_r.at[1, p], gdev(3))

    slot1, slot2, slot3 = pl.ds(512, 512), pl.ds(1024, 512), pl.ds(1536, 512)
    first, second = pl.ds(0, OWN), pl.ds(OWN, OWN)

    def near(p):
        send(GO.at[block(1, p, 0, BLK)], G.at[p, :, slot2], nbr_s.at[0], blk_r.at[p], gdev(1))
        send(GO.at[block(3, p, 0, BLK)], G.at[p, :, slot1], nbr_s.at[1], blk_r.at[p], gdev(3))

    def hop_relay(p):
        wait(RB.at[0, p], hop_r.at[0, p])
        send(RB.at[0, p], G.at[p, first, slot3], rel_s.at[0], blk_r.at[p], gdev(1))
        wait(RB.at[1, p], hop_r.at[1, p])
        send(RB.at[1, p], G.at[p, second, slot3], rel_s.at[1], blk_r.at[p], gdev(3))

    def block_done(p):
        own_copies[p].wait()
        wait(G.at[p, :, pl.ds(512, 1536)], blk_r.at[p])

    hop(0)
    hop(1)
    q_near(1)
    y_own(1, 0)
    q_far(0)
    y_own(0, 1)
    for cp in own_copies:
        cp.start()
    q_far(1)
    y_own(1, 1)
    q_relay(2)
    for p in range(2, 4):
        hop(p)
    near(0)

    def y_both(u):
        y_own(u, 0)
        y_own(u, 1)

    y_both(2)
    y_relay(0)
    q_near(2)
    q_far(2)
    y_both(3)
    hop_relay(0)
    near(1)
    hop_relay(1)
    near(2)
    y_relay(1)
    hop_relay(2)
    near(3)
    hop_relay(3)
    q_own(3, 0)
    q_own(3, 1)
    y_relay(2)
    y_both(4)
    y_relay(3)
    y_both(5)
    y_relay(4)
    y_both(6)

    for p in range(3):
        block_done(p)
    acc[...] = jnp.zeros_like(acc)

    def out_tile(h, t):
        return pl.ds(pl.multiple_of(h * HALF + t * TILE, TILE), TILE)

    def product(p, n, t):
        acts = A[:, :, :, :, tile(t)].reshape(4 * 512, TILE)
        left = G[p : p + n].reshape(n * BLK, 2048)
        return jnp.dot(left, acts, preferred_element_type=F32).astype(BF).reshape(n, BLK, TILE)

    def reduce_send(d, part, core, t):
        src = PB.at[1 + d, pl.ds(part * OWN, OWN), tile(t)]
        send(src, RF.at[d, :, out_tile(c, t)], rf_s.at[d, core], fin_r.at[t], rdev(1 + 2 * d, core))

    def add_send(t):
        for d in (0, 1):
            wait(H.at[d, :, tile(t)], rh_r.at[d, t])
            rows = pl.ds(d * OWN, OWN)
            total = PB[1 + d, rows, tile(t)].astype(F32) + H[d, :, tile(t)].astype(F32)
            PB[1 + d, rows, tile(t)] = total.astype(BF)
            reduce_send(d, d, d, t)

    keep = of(c * OWN, OWN)
    give = of((1 - c) * OWN, OWN)

    def own_block(t):
        PB[3, :, tile(t)] = product(3, 1, t)[0]
        send(PB.at[3, give, tile(t)], PP.at[:, out_tile(c, t)], pp_s.at[0], fin_r.at[t], partner)
        PP[:, out_tile(c, t)] = PB[3, keep, tile(t)]

    def copy_out(h, t):
        cols = out_tile(h, t)
        return pltpu.make_async_copy(GR.at[:, cols], grad_out.at[:, cols], out_sem.at[0])

    def finish(t):
        wait(RF.at[0, :, pl.ds(0, 5 * TILE)], fin_r.at[t])
        for h in (0, 1):
            cols = out_tile(h, t)
            g = PP[:, cols].astype(F32) + RF[0, :, cols].astype(F32) + RF[1, :, cols].astype(F32)
            GR[:, cols] = g
            copy_out(h, t).start()
            sq = jnp.sum((g * g).reshape(OWN // 8, 8, TILE), axis=0)
            acc[...] += sq[:, :128] + sq[:, 128:]

    def relay_and_send(u):
        y_relay(u)
        if u + 2 < STEPS:
            y_both(u + 2)

    def last_arrivals():
        q_near(3)
        q_far(3)

    def step(t, _):
        pl.when(t < STEPS - 2)(functools.partial(y_done, t))
        pl.when(t == STEPS - 2)(last_arrivals)
        pl.when(t >= STEPS - 2)(functools.partial(y_near, t))
        PB[0:3, :, tile(t)] = product(0, 3, t)
        send(PB.at[0, first, tile(t)], H.at[0, :, tile(t)], rh_s.at[0], rh_r.at[0, t], rdev(1, c))
        send(PB.at[0, second, tile(t)], H.at[1, :, tile(t)], rh_s.at[1], rh_r.at[1, t], rdev(3, c))
        reduce_send(0, 1, 1, t)
        reduce_send(1, 0, 0, t)

        pl.when(t == 2)(functools.partial(block_done, 3))
        pl.when(t >= 2)(functools.partial(own_block, t - 2))
        pl.when(t >= 1)(functools.partial(add_send, t - 1))
        pl.when(t >= 3)(functools.partial(finish, t - 3))
        pl.when(t == 1)(functools.partial(relay_and_send, 5))
        pl.when(t == 3)(functools.partial(q_relay, 3))
        return 0

    lax.fori_loop(0, STEPS, step, 0)
    own_block(STEPS - 2)
    own_block(STEPS - 1)
    finish(STEPS - 3)
    add_send(STEPS - 1)
    finish(STEPS - 2)
    finish(STEPS - 1)

    me = ((z * 4 + x) * 2 + c) * 4 + y
    NS[0] = jnp.sum(acc[...], axis=0, keepdims=True)
    N1[me] = NS[0]

    planes = [lax.rem(y + k, 4) for k in (2, 1, 3, 0)]

    def tell(dz, dx):
        for dc in (1, 0):
            for dy, plane in zip((2, 1, 3, 0), planes):
                if dz or dx or dc or dy:
                    dev = (lax.rem(z + dz, 4), lax.rem(x + dx, 4), lax.rem(c + dc, 2), plane)
                    send(NS.at[0], N1.at[me], n_s.at[0], n_r.at[0], dev)

    for hops in (4, 3, 2, 1, 0):
        for dz in (2, 1, 3, 0):
            for dx in (2, 1, 3, 0):
                if min(dz, 4 - dz) + min(dx, 4 - dx) == hops:
                    tell(dz, dx)

    for i in range(2):
        wait(S.at[:, :, pieces[i]], pair_s.at[i])
    wait(half, pair_s.at[2])
    q_drain()
    for d in (0, 1):
        wait(RB.at[d], hop_s.at[d])
        wait(RB.at[d], rel_s.at[d])
        wait(G.at[:, :, slot1], nbr_s.at[d])
        wait(H.at[d], rh_s.at[d])
        for core in (0, 1):
            wait(H.at[d], rf_s.at[d, core])
    wait(H.at[0], pp_s.at[0])
    wait(GR, out_sem.at[0])
    y_drain()
    others = N1.at[pl.ds(0, 127)]
    wait(others, n_r.at[0])
    total = jnp.sum(jnp.sum(N1[...], axis=0), keepdims=True)
    limit = clip_rms * jnp.sqrt(jnp.full((1, 1), FF * ROWS, F32))
    factor_out[...] = jnp.broadcast_to(jnp.minimum(1.0, limit / jnp.sqrt(total)), (8, 128))
    wait(others, n_s.at[0])


def adam_kernel(factor, grad, moment, second, master, nm_out, ns_out, nw_out, w_out, nm, ns, nw, w, sems):
    f = factor[0:1, 0:1]
    pairs = ((nm, nm_out), (ns, ns_out), (nw, nw_out), (w, w_out))

    def step(i, _):
        rows = pl.ds(pl.multiple_of(i * 16, 16), 16)
        clipped = f * grad[rows, :]
        new_moment = beta_first * moment[rows, :] + (1.0 - beta_first) * clipped
        new_second = beta_second * second[rows, :] + (1.0 - beta_second) * clipped * clipped
        new_master = master[rows, :] - learn_rate * new_moment / (jnp.sqrt(new_second) + adam_eps)
        nm[rows, :] = new_moment
        ns[rows, :] = new_second
        nw[rows, :] = new_master
        w[rows, :] = new_master.astype(BF)
        for k, (src, dst) in enumerate(pairs):
            pltpu.make_async_copy(src.at[rows], dst.at[rows], sems.at[k]).start()
        return 0

    lax.fori_loop(0, OWN // 16, step, 0)
    for k, (src, dst) in enumerate(pairs):
        pltpu.make_async_copy(src, dst, sems.at[k]).wait()


def adam(factor, grad, moment, second, master):
    vmem = pltpu.VMEM
    shape = (OWN, ROWS)
    kinds = (F32, F32, F32, BF)
    return pl.pallas_call(
        adam_kernel,
        out_shape=tuple(jax.ShapeDtypeStruct(shape, kind) for kind in kinds),
        in_specs=[pl.BlockSpec(memory_space=vmem)] * 5,
        out_specs=tuple(pl.BlockSpec(memory_space=pltpu.HBM) for _ in kinds),
        scratch_shapes=[vmem(shape, kind) for kind in kinds] + [pltpu.SemaphoreType.DMA((4,))],
        compiler_params=pltpu.CompilerParams(vmem_limit_bytes=24 * 1024 * 1024),
        cost_estimate=pl.CostEstimate(flops=20 * OWN * ROWS, bytes_accessed=30 * OWN * ROWS, transcendentals=OWN * ROWS),
        name="adam",
    )(factor, grad, moment, second, master)


def owned_gradient(activations, out_grads, act_scale, grad_scale):
    dma = pltpu.SemaphoreType.DMA
    vmem = pltpu.VMEM
    scratch = [
        vmem((2, 128, ROWS), BF),
        vmem((2, 128, 5120), BF),
        vmem((2, ROWS // 128), BF),
        vmem((2, 5120), BF),
        vmem((2, ROWS), F32),
        vmem((4, 2, 4, 64, HALF), BF),
        vmem((4, 64, HALF), BF),
        vmem((5120, 512), BF),
        vmem((4, BLK, 2048), BF),
        vmem((2, 4, OWN, 512), BF),
        vmem((4, BLK, HALF), BF),
        vmem((2, OWN, HALF), BF),
        vmem((2, OWN, ROWS), BF),
        vmem((OWN, ROWS), BF),
        vmem((OWN, ROWS), F32),
        vmem((8, 128), F32),
        vmem((1, 1, 128), F32),
        vmem((128, 1, 128), F32),
        dma((4,)),
        dma((4,)),
        dma((3,)), dma((3,)),
        dma((6, 2)), dma((4, 3, 2)),
        dma((3, 2)), dma((STEPS, 3)),
        dma((2,)), dma((2, 4)),
        dma((2,)), dma((2,)), dma((4,)),
        dma((2,)), dma((2, STEPS)),
        dma((2, 2)), dma((1,)), dma((STEPS,)),
        dma((1,)),
        dma((1,)), dma((1,)),
    ]
    return pl.pallas_call(
        kernel,
        out_shape=(
            jax.ShapeDtypeStruct((OWN, ROWS), F32),
            jax.ShapeDtypeStruct((8, 128), F32),
        ),
        in_specs=[pl.BlockSpec(memory_space=pltpu.HBM)] * 4,
        out_specs=(pl.BlockSpec(memory_space=pl.ANY), pl.BlockSpec(memory_space=vmem)),
        scratch_shapes=scratch,
        compiler_params=pltpu.CompilerParams(
            collective_id=0, has_side_effects=True, vmem_limit_bytes=46 * 1024 * 1024
        ),
        cost_estimate=pl.CostEstimate(
            flops=2 * 8192 * OWN * ROWS, bytes_accessed=8 * 1024 * 1024, transcendentals=0
        ),
        name="owned_gradient",
    )(*(
        pltpu.with_memory_space_constraint(v, pltpu.HBM)
        for v in (activations, out_grads, act_scale, grad_scale.reshape(2, 5120))
    ))


def per_device(activations, out_grads, act_scale, grad_scale, moment, second, master):
    grad_owned, factors = owned_gradient(activations, out_grads, act_scale, grad_scale)
    return adam(factors, grad_owned, moment, second, master)


def solution(mesh):
    finer = Mesh(
        mesh.devices.reshape(4, 4, 2, mesh.shape["tensor"]), ("dp_0", "dp_1", "dp_2", "tensor")
    )
    in_specs = (
        P(DP, None, None),
        P(DP, None, "tensor"),
        P(DP, None),
        P(DP, None, "tensor"),
        P(TENSOR_DP, None),
        P(TENSOR_DP, None),
        P(TENSOR_DP, None),
    )
    out_specs = (P(TENSOR_DP, None), P(TENSOR_DP, None), P(TENSOR_DP, None), P(TENSOR_DP, None))
    return jax.shard_map(
        per_device, mesh=finer, in_specs=in_specs, out_specs=out_specs, check_vma=False
    )
```

```python
import functools

import jax
import jax.numpy as jnp
from jax import lax
from jax.experimental import pallas as pl
from jax.experimental.pallas import tpu as pltpu
from jax.sharding import Mesh
from jax.sharding import PartitionSpec as P

FF = 20480
ROWS = 4096
DP = ("dp_0", "dp_1", "dp_2")
TENSOR_DP = ("tensor", "dp_0", "dp_1", "dp_2")

clip_rms = 1.0
beta_first = 0.9
beta_second = 0.95
learn_rate = 0.003
adam_eps = 1e-08

TOK = 256
HALF = ROWS // 2
TILE = 256
STEPS = HALF // TILE
BLK = 320
OWN = 160
QUART = 128
B_OFF = (2, 1, 3, 0)
BF = jnp.bfloat16
F32 = jnp.float32


def kernel(
    acts_hbm, grads_hbm, ascale_hbm, gscale_hbm,
    grad_out, factor_out,
    acts_raw, grads_raw, ascale, gscale, wide, A, S, GO, G, RB, PB, H, RF, PP, GR, acc, NS, N1,
    load_sem, own_sem, pair_s, pair_r, q_s, q_r, y_s, y_r,
    hop_s, hop_r, nbr_s, rel_s, blk_r,
    rh_s, rh_r, rf_s, pp_s, fin_r, out_sem, n_s, n_r,
):
    z = lax.axis_index("dp_0")
    x = lax.axis_index("dp_1")
    c = lax.axis_index("dp_2")
    y = lax.axis_index("tensor")
    a = x + c * (z - x)
    b = z + c * (x - z)

    def gdev(d):
        return (lax.rem(z + c * d, 4), lax.rem(x + (1 - c) * d, 4), c, y)

    def rdev(d, core):
        return (lax.rem(z + (1 - c) * d, 4), lax.rem(x + c * d, 4), core, y)

    def ydev(d):
        return (z, x, c, lax.rem(y + d, 4))

    partner = (z, x, 1 - c, y)
    MESH = pl.DeviceIdType.MESH

    def send(src, dst, ss, rs, dev):
        pltpu.make_async_remote_copy(
            src_ref=src, dst_ref=dst, send_sem=ss, recv_sem=rs, device_id=dev, device_id_type=MESH
        ).start()

    def wait(ref, sem):
        pltpu.make_async_copy(ref, ref, sem).wait()

    def of(i, n):
        return pl.ds(pl.multiple_of(i, n), n)

    loads = [
        pltpu.make_async_copy(src, dst, load_sem.at[i])
        for i, (src, dst) in enumerate(
            ((ascale_hbm, ascale), (acts_hbm, acts_raw), (gscale_hbm, gscale), (grads_hbm, grads_raw))
        )
    ]
    for k in (1, 0, 3, 2):
        loads[k].start()

    barrier = pltpu.get_barrier_semaphore()
    greet = [partner]
    for d in (1, 3):
        for core in (0, 1):
            greet.append((lax.rem(z + d, 4), x, core, y))
            greet.append((z, lax.rem(x + d, 4), core, y))
        greet.append(ydev(d))
    for dev in greet:
        pl.semaphore_signal(barrier, inc=1, device_id=dev, device_id_type=MESH)
    loads[0].wait()
    for r in range(ROWS // 128):
        wide[:, r * 128 : (r + 1) * 128] = jnp.broadcast_to(
            ascale[:, r : r + 1].astype(F32), (2, 128)
        )
    loads[1].wait()

    def scale_step(i, _):
        dst = pl.ds(pl.multiple_of(i * 512, 512), 512)
        for which, put in ((1 - c, 0), (c, 1)):
            cols = pl.ds(pl.multiple_of(which * HALF + i * 512, 512), 512)
            for blk in range(2):
                v = (acts_raw[blk, :, cols].astype(F32) * wide[blk : blk + 1, cols]).astype(BF)
                v = v.reshape(2, 64, 512)
                rows = pl.ds(2 * blk, 2)
                if put:
                    A[0, c, rows, :, dst] = v
                else:
                    S[rows, :, dst] = v
        return 0

    lax.fori_loop(0, HALF // 512, scale_step, 0)

    def turn(i, _):
        cols = pl.ds(pl.multiple_of(i * 512, 512), 512)
        for blk in range(2):
            v = grads_raw[blk, :, cols].astype(F32) * gscale[blk : blk + 1, cols].astype(F32)
            GO[cols, of(c * TOK + blk * 128, 128)] = v.T.astype(BF)
        return 0

    pl.semaphore_wait(barrier, len(greet))

    far = lax.rem(y + 2, 4)
    last_tiles = pl.ds(HALF - 2 * TILE, 2 * TILE)
    groups = (
        (pl.ds(0, TILE), y),
        (pl.ds(TILE, 2 * TILE), y),
        (pl.ds(3 * TILE, HALF - 3 * TILE), y),
        (last_tiles, far),
    )
    pieces = (pl.ds(0, TILE), pl.ds(TILE, HALF - TILE))
    def q_own(g, k):
        cols, q = groups[g]
        e = 3 * (g // 3)
        who = c + k * (1 - 2 * c)
        src = A.at[0, who, q, :, cols]
        send(src, A.at[2, who, q, :, cols], q_s.at[e, k], q_r.at[g, 0, who], gdev(1))
        send(src, A.at[1, who, q, :, cols], q_s.at[e + 1, k], q_r.at[g, 1, who], gdev(3))

    def first_group():
        cols, q = groups[0]
        q_own(0, 0)
        src = S.at[q, :, cols]
        send(src, A.at[2, c, q, :, cols], q_s.at[0, 1], q_r.at[0, 0, c], rdev(1, 1 - c))
        send(src, A.at[1, c, q, :, cols], q_s.at[1, 1], q_r.at[0, 1, c], rdev(3, 1 - c))

    def q_relay(g):
        cols, q = groups[g]
        e = 3 * (g // 3) + 2
        wait(A.at[2, 0, q, :, cols], q_r.at[g, 0, 0])
        send(A.at[2, 0, q, :, cols], A.at[3, 0, q, :, cols], q_s.at[e, 0], q_r.at[g, 2, 0], gdev(1))
        wait(A.at[1, 1, q, :, cols], q_r.at[g, 1, 1])
        send(A.at[1, 1, q, :, cols], A.at[3, 1, q, :, cols], q_s.at[e, 1], q_r.at[g, 2, 1], gdev(3))

    def q_near(g):
        cols, q = groups[g]
        wait(A.at[2, 1, q, :, cols], q_r.at[g, 0, 1])
        wait(A.at[1, 0, q, :, cols], q_r.at[g, 1, 0])

    def q_far(g):
        cols, q = groups[g]
        wait(A.at[3, 0, q, :, cols], q_r.at[g, 2, 0])
        wait(A.at[3, 1, q, :, cols], q_r.at[g, 2, 1])

    def q_drain():
        for i in range(3):
            for k in range(2):
                wait(A.at[0, 0, y], q_s.at[i, k])
                wait(A.at[0, 0, y, :, last_tiles], q_s.at[3 + i, k])

    def tile(t):
        return pl.ds(pl.multiple_of(t * TILE, TILE), TILE)

    parts = (pl.ds(1, 2), pl.ds(3, 1))
    both = pl.ds(0, 2)
    below = lax.rem(y + 3, 4)
    above = lax.rem(y + 1, 4)

    def y_own(u, i):
        v = A.at[parts[i], both, y, :, tile(u)]
        send(v, v, y_s.at[i, 0], y_r.at[u, 0], ydev(1))
        send(v, v, y_s.at[i, 1], y_r.at[u, 0], ydev(3))

    three = pl.ds(1, 3)

    def y_relay(u):
        y_near(u)
        v = A.at[three, 0, below, :, tile(u)]
        send(v, v, y_s.at[2, 0], y_r.at[u, 1], ydev(1))
        v = A.at[three, 1, above, :, tile(u)]
        send(v, v, y_s.at[2, 1], y_r.at[u, 1], ydev(3))

    def y_done(u):
        wait(A.at[three, both, far, :, tile(u)], y_r.at[u, 1])

    def y_drain():
        for k in range(2):
            for i in range(2):
                wait(A.at[parts[i], both, y], y_s.at[i, k])
            wait(A.at[three, 0, y, :, pl.ds(0, HALF - 2 * TILE)], y_s.at[2, k])

    def y_near(u):
        wait(A.at[three, both, both, :, tile(u)], y_r.at[u, 0])

    first_group()
    for i in range(2):
        send(S.at[:, :, pieces[i]], A.at[0, c, :, :, pieces[i]], pair_s.at[i], pair_r.at[i], partner)
    q_own(1, 0)
    q_own(2, 0)
    wait(A.at[0, 1 - c, :, :, pieces[0]], pair_r.at[0])

    loads[2].wait()
    loads[3].wait()
    lax.fori_loop(0, 10, turn, 0)
    half = GO.at[:, of(c * TOK, TOK)]
    send(half, half, pair_s.at[2], pair_r.at[2], partner)
    wait(A.at[0, 1 - c, :, :, pieces[1]], pair_r.at[1])
    q_own(1, 1)
    q_own(2, 1)
    q_relay(0)
    q_near(0)
    y_own(0, 0)
    q_relay(1)

    def block(da, p, part, n):
        aa = lax.rem(a + da, 4)
        bb = lax.rem(b + B_OFF[p], 4)
        start = (bb * 4 + aa + c * 3 * (aa - bb)) * BLK + part * OWN
        return pl.ds(pl.multiple_of(start, OWN), n)

    wait(GO.at[:, of((1 - c) * TOK, TOK)], pair_r.at[2])
    own_copies = [
        pltpu.make_async_copy(GO.at[block(0, p, 0, BLK)], G.at[p, :, pl.ds(0, 512)], own_sem.at[p])
        for p in range(4)
    ]

    def hop(p):
        send(GO.at[block(2, p, 0, OWN)], RB.at[0, p], hop_s.at[0], hop_r.at[0, p], gdev(1))
        send(GO.at[block(2, p, 1, OWN)], RB.at[1, p], hop_s.at[1], hop_r.at[1, p], gdev(3))

    slot1, slot2, slot3 = pl.ds(512, 512), pl.ds(1024, 512), pl.ds(1536, 512)
    first, second = pl.ds(0, OWN), pl.ds(OWN, OWN)

    def near(p):
        send(GO.at[block(1, p, 0, BLK)], G.at[p, :, slot2], nbr_s.at[0], blk_r.at[p], gdev(1))
        send(GO.at[block(3, p, 0, BLK)], G.at[p, :, slot1], nbr_s.at[1], blk_r.at[p], gdev(3))

    def hop_relay(p):
        wait(RB.at[0, p], hop_r.at[0, p])
        send(RB.at[0, p], G.at[p, first, slot3], rel_s.at[0], blk_r.at[p], gdev(1))
        wait(RB.at[1, p], hop_r.at[1, p])
        send(RB.at[1, p], G.at[p, second, slot3], rel_s.at[1], blk_r.at[p], gdev(3))

    def block_done(p):
        own_copies[p].wait()
        wait(G.at[p, :, pl.ds(512, 1536)], blk_r.at[p])

    hop(0)
    hop(1)
    q_near(1)
    y_own(1, 0)
    q_far(0)
    y_own(0, 1)
    for cp in own_copies:
        cp.start()
    q_far(1)
    y_own(1, 1)
    q_relay(2)
    for p in range(2, 4):
        hop(p)
    near(0)

    def y_both(u):
        y_own(u, 0)
        y_own(u, 1)

    y_both(2)
    y_relay(0)
    q_near(2)
    q_far(2)
    y_both(3)
    hop_relay(0)
    near(1)
    hop_relay(1)
    near(2)
    y_relay(1)
    hop_relay(2)
    near(3)
    hop_relay(3)
    q_own(3, 0)
    q_own(3, 1)
    y_relay(2)
    y_both(4)
    y_relay(3)
    y_both(5)
    y_relay(4)
    y_both(6)

    for p in range(3):
        block_done(p)
    acc[...] = jnp.zeros_like(acc)

    def out_tile(h, t):
        return pl.ds(pl.multiple_of(h * HALF + t * TILE, TILE), TILE)

    def product(p, n, t):
        acts = A[:, :, :, :, tile(t)].reshape(4 * 512, TILE)
        left = G[p : p + n].reshape(n * BLK, 2048)
        return jnp.dot(left, acts, preferred_element_type=F32).astype(BF).reshape(n, BLK, TILE)

    def reduce_send(d, part, core, t):
        src = PB.at[1 + d, pl.ds(part * OWN, OWN), tile(t)]
        send(src, RF.at[d, :, out_tile(c, t)], rf_s.at[d, core], fin_r.at[t], rdev(1 + 2 * d, core))

    def add_send(t):
        wait(H.at[:, :, tile(t)], rh_r.at[t])
        for d in (0, 1):
            rows = pl.ds(d * OWN, OWN)
            total = PB[1 + d, rows, tile(t)].astype(F32) + H[d, :, tile(t)].astype(F32)
            PB[1 + d, rows, tile(t)] = total.astype(BF)
            reduce_send(d, d, d, t)

    keep = of(c * OWN, OWN)
    give = of((1 - c) * OWN, OWN)

    def own_block(t):
        PB[3, :, tile(t)] = product(3, 1, t)[0]
        send(PB.at[3, give, tile(t)], PP.at[:, out_tile(c, t)], pp_s.at[0], fin_r.at[t], partner)
        PP[:, out_tile(c, t)] = PB[3, keep, tile(t)]

    def copy_out(h, t):
        cols = out_tile(h, t)
        return pltpu.make_async_copy(GR.at[:, cols], grad_out.at[:, cols], out_sem.at[0])

    def finish(t):
        wait(RF.at[0, :, pl.ds(0, 5 * TILE)], fin_r.at[t])
        for h in (0, 1):
            cols = out_tile(h, t)
            g = PP[:, cols].astype(F32) + RF[0, :, cols].astype(F32) + RF[1, :, cols].astype(F32)
            GR[:, cols] = g
            copy_out(h, t).start()
            sq = jnp.sum((g * g).reshape(OWN // 8, 8, TILE), axis=0)
            acc[...] += sq[:, :128] + sq[:, 128:]

    def relay_and_send(u):
        y_relay(u)
        if u + 2 < STEPS:
            y_both(u + 2)

    def last_arrivals():
        q_near(3)
        q_far(3)

    def step(t, _):
        pl.when(t < STEPS - 2)(functools.partial(y_done, t))
        pl.when(t == STEPS - 2)(last_arrivals)
        pl.when(t >= STEPS - 2)(functools.partial(y_near, t))
        PB[0:3, :, tile(t)] = product(0, 3, t)
        send(PB.at[0, first, tile(t)], H.at[0, :, tile(t)], rh_s.at[0], rh_r.at[t], rdev(1, c))
        send(PB.at[0, second, tile(t)], H.at[1, :, tile(t)], rh_s.at[1], rh_r.at[t], rdev(3, c))
        reduce_send(0, 1, 1, t)
        reduce_send(1, 0, 0, t)

        pl.when(t == 2)(functools.partial(block_done, 3))
        pl.when(t >= 2)(functools.partial(own_block, t - 2))
        pl.when(t >= 1)(functools.partial(add_send, t - 1))
        pl.when(t >= 3)(functools.partial(finish, t - 3))
        pl.when(t == 1)(functools.partial(relay_and_send, 5))
        pl.when(t == 3)(functools.partial(q_relay, 3))
        return 0

    lax.fori_loop(0, STEPS, step, 0)
    own_block(STEPS - 2)
    own_block(STEPS - 1)
    finish(STEPS - 3)
    add_send(STEPS - 1)
    finish(STEPS - 2)
    finish(STEPS - 1)

    me = ((z * 4 + x) * 2 + c) * 4 + y
    NS[0] = jnp.sum(acc[...], axis=0, keepdims=True)
    N1[me] = NS[0]

    planes = [lax.rem(y + k, 4) for k in (2, 1, 3, 0)]

    def tell(dz, dx):
        for dc in (1, 0):
            for dy, plane in zip((2, 1, 3, 0), planes):
                if dz or dx or dc or dy:
                    dev = (lax.rem(z + dz, 4), lax.rem(x + dx, 4), lax.rem(c + dc, 2), plane)
                    send(NS.at[0], N1.at[me], n_s.at[0], n_r.at[0], dev)

    for hops in (4, 3, 2, 1, 0):
        for dz in (2, 1, 3, 0):
            for dx in (2, 1, 3, 0):
                if min(dz, 4 - dz) + min(dx, 4 - dx) == hops:
                    tell(dz, dx)

    for i in range(2):
        wait(S.at[:, :, pieces[i]], pair_s.at[i])
    wait(half, pair_s.at[2])
    q_drain()
    for d in (0, 1):
        wait(RB.at[d], hop_s.at[d])
        wait(RB.at[d], rel_s.at[d])
        wait(G.at[:, :, slot1], nbr_s.at[d])
        wait(H.at[d], rh_s.at[d])
        for core in (0, 1):
            wait(H.at[d], rf_s.at[d, core])
    wait(H.at[0], pp_s.at[0])
    wait(GR, out_sem.at[0])
    y_drain()
    others = N1.at[pl.ds(0, 127)]
    wait(others, n_r.at[0])
    total = jnp.sum(jnp.sum(N1[...], axis=0), keepdims=True)
    limit = clip_rms * jnp.sqrt(jnp.full((1, 1), FF * ROWS, F32))
    factor_out[...] = jnp.broadcast_to(jnp.minimum(1.0, limit / jnp.sqrt(total)), (8, 128))
    wait(others, n_s.at[0])


def adam_kernel(factor, grad, moment, second, master, nm_out, ns_out, nw_out, w_out, nm, ns, nw, w, sems):
    f = factor[0:1, 0:1]
    pairs = ((nm, nm_out), (ns, ns_out), (nw, nw_out), (w, w_out))

    def step(i, _):
        rows = pl.ds(pl.multiple_of(i * 16, 16), 16)
        clipped = f * grad[rows, :]
        new_moment = beta_first * moment[rows, :] + (1.0 - beta_first) * clipped
        new_second = beta_second * second[rows, :] + (1.0 - beta_second) * clipped * clipped
        new_master = master[rows, :] - learn_rate * new_moment / (jnp.sqrt(new_second) + adam_eps)
        nm[rows, :] = new_moment
        ns[rows, :] = new_second
        nw[rows, :] = new_master
        w[rows, :] = new_master.astype(BF)
        for k, (src, dst) in enumerate(pairs):
            pltpu.make_async_copy(src.at[rows], dst.at[rows], sems.at[k]).start()
        return 0

    lax.fori_loop(0, OWN // 16, step, 0)
    for k, (src, dst) in enumerate(pairs):
        pltpu.make_async_copy(src, dst, sems.at[k]).wait()


def adam(factor, grad, moment, second, master):
    vmem = pltpu.VMEM
    shape = (OWN, ROWS)
    kinds = (F32, F32, F32, BF)
    return pl.pallas_call(
        adam_kernel,
        out_shape=tuple(jax.ShapeDtypeStruct(shape, kind) for kind in kinds),
        in_specs=[pl.BlockSpec(memory_space=vmem)] * 5,
        out_specs=tuple(pl.BlockSpec(memory_space=pltpu.HBM) for _ in kinds),
        scratch_shapes=[vmem(shape, kind) for kind in kinds] + [pltpu.SemaphoreType.DMA((4,))],
        compiler_params=pltpu.CompilerParams(vmem_limit_bytes=24 * 1024 * 1024),
        cost_estimate=pl.CostEstimate(flops=20 * OWN * ROWS, bytes_accessed=30 * OWN * ROWS, transcendentals=OWN * ROWS),
        name="adam",
    )(factor, grad, moment, second, master)


def owned_gradient(activations, out_grads, act_scale, grad_scale):
    dma = pltpu.SemaphoreType.DMA
    vmem = pltpu.VMEM
    scratch = [
        vmem((2, 128, ROWS), BF),
        vmem((2, 128, 5120), BF),
        vmem((2, ROWS // 128), BF),
        vmem((2, 5120), BF),
        vmem((2, ROWS), F32),
        vmem((4, 2, 4, 64, HALF), BF),
        vmem((4, 64, HALF), BF),
        vmem((5120, 512), BF),
        vmem((4, BLK, 2048), BF),
        vmem((2, 4, OWN, 512), BF),
        vmem((4, BLK, HALF), BF),
        vmem((2, OWN, HALF), BF),
        vmem((2, OWN, ROWS), BF),
        vmem((OWN, ROWS), BF),
        vmem((OWN, ROWS), F32),
        vmem((8, 128), F32),
        vmem((1, 1, 128), F32),
        vmem((128, 1, 128), F32),
        dma((4,)),
        dma((4,)),
        dma((3,)), dma((3,)),
        dma((6, 2)), dma((4, 3, 2)),
        dma((3, 2)), dma((STEPS, 2)),
        dma((2,)), dma((2, 4)),
        dma((2,)), dma((2,)), dma((4,)),
        dma((2,)), dma((STEPS,)),
        dma((2, 2)), dma((1,)), dma((STEPS,)),
        dma((1,)),
        dma((1,)), dma((1,)),
    ]
    return pl.pallas_call(
        kernel,
        out_shape=(
            jax.ShapeDtypeStruct((OWN, ROWS), F32),
            jax.ShapeDtypeStruct((8, 128), F32),
        ),
        in_specs=[pl.BlockSpec(memory_space=pltpu.HBM)] * 4,
        out_specs=(pl.BlockSpec(memory_space=pl.ANY), pl.BlockSpec(memory_space=vmem)),
        scratch_shapes=scratch,
        compiler_params=pltpu.CompilerParams(
            collective_id=0, has_side_effects=True, vmem_limit_bytes=46 * 1024 * 1024
        ),
        cost_estimate=pl.CostEstimate(
            flops=2 * 8192 * OWN * ROWS, bytes_accessed=8 * 1024 * 1024, transcendentals=0
        ),
        name="owned_gradient",
    )(*(
        pltpu.with_memory_space_constraint(v, pltpu.HBM)
        for v in (activations, out_grads, act_scale, grad_scale.reshape(2, 5120))
    ))


def per_device(activations, out_grads, act_scale, grad_scale, moment, second, master):
    grad_owned, factors = owned_gradient(activations, out_grads, act_scale, grad_scale)
    return adam(factors, grad_owned, moment, second, master)


def solution(mesh):
    finer = Mesh(
        mesh.devices.reshape(4, 4, 2, mesh.shape["tensor"]), ("dp_0", "dp_1", "dp_2", "tensor")
    )
    in_specs = (
        P(DP, None, None),
        P(DP, None, "tensor"),
        P(DP, None),
        P(DP, None, "tensor"),
        P(TENSOR_DP, None),
        P(TENSOR_DP, None),
        P(TENSOR_DP, None),
    )
    out_specs = (P(TENSOR_DP, None), P(TENSOR_DP, None), P(TENSOR_DP, None), P(TENSOR_DP, None))
    return jax.shard_map(
        per_device, mesh=finer, in_specs=in_specs, out_specs=out_specs, check_vma=False
    )
```
